128 devices in a mesh: lon: 8 (over z, core), lat: 4 (over y), mem: 4 (over x).
Axes of the slice: x: 4, y: 4, z: 4, core: 2. Of those that a mesh axis runs over, the one named last changes fastest.
Arguments:
- ensemble: bfloat16 [80, 4, 4, 512, 512], P('mem', None, None, 'lon', 'lat'), may hold values from -6 to 6
- huber: float32 [4, 4, 512, 512], P(None, None, 'lon', 'lat'), may hold values from 0.1 to 1
- innovation: float32 [4, 4, 512, 512], P(None, None, 'lon', 'lat'), may hold values from -6 to 6
- sea_mask: int32 [128, 128], P('lon', 'lat'), may hold values 0 or 1
Outputs:
- control: float32 [80, 4, 128, 128], P('mem', None, 'lon', 'lat')
- gradient: float32 [80, 4, 128, 128], P('mem', None, 'lon', 'lat')
The draws below stay inside these ranges and needn't reach their ends.
All inputs are finite; a program needn't handle non-finite values. No bound on the sum of `sea_mask` on one device may be relied on, other than what follows from the above.
Results may differ from the reference program's by a relative error of at most 0.013.
Values may be sent and summed in bfloat16 or wider, within the bound.
A program may use at most 128 MiB of HBM per device.

```python
import math
import jax
import jax.numpy as jnp
from jax import lax

MEMBERS = 80
VARS = 4
RATIO = 4
DSTEPS = 4
ITERS = 3
LEV = 4
NX = 512
NY = 512
NCX = 128
NCY = 128


def place_ends(result, key, low, top_value):
    longest = result.shape.index(max(result.shape))
    spots = []
    for shift in (0, 1):
        where = [jax.random.randint(jax.random.fold_in(key, axis), (), 0, length) for axis, length in enumerate(result.shape)]
        where[longest] = (where[longest] + shift) % result.shape[longest]
        spots.append(tuple(where))
    return result.at[spots[0]].set(low).at[spots[1]].set(top_value)


def levels(key, dims, pieces, smallest, high):
    gain = 1.0
    for axis_at, shards_of in pieces:
        heights = jax.random.uniform(jax.random.fold_in(jax.random.fold_in(key, 6), axis_at), (shards_of,), jnp.float32, smallest / len(pieces), high / len(pieces))
        gain = gain * jnp.repeat(jnp.exp(heights), dims[axis_at] // shards_of).reshape((-1,) + (1,) * (len(dims) - 1 - axis_at))
    return gain


def bell_draw(own_key, dims, width, limit, shards=(), kind=jnp.bfloat16):
    array = width * jax.random.normal(own_key, dims, jnp.float32)
    if shards:
        array = array * levels(own_key, dims, shards, -0.22, 0.18)
    return jnp.clip(array, -limit, limit).astype(kind)


def setup_inputs(seed: int = 0) -> dict:
    streams_of = jax.random.split(jax.random.key(seed), 5)
    return {
        "ensemble": bell_draw(streams_of[0], (MEMBERS, VARS, LEV, NX, NY), 1.0, 6.0, ((0, 4), (3, 8), (4, 4))),
        "huber": jnp.clip(jnp.exp(math.log(1.0) - 2.3025851 * jax.random.uniform(streams_of[1], (VARS, LEV, NX, NY), jnp.float32) ** levels(streams_of[1], (VARS, LEV, NX, NY), ((2, 8), (3, 4)), -0.2, 0.2)), 0.1, 1.0),
        "innovation": bell_draw(streams_of[2], (VARS, LEV, NX, NY), 1.0, 6.0, ((2, 8), (3, 4)), jnp.float32),
        "sea_mask": place_ends((jax.random.randint(streams_of[3], (NCX, NCY), 0, 4) < 3).astype(jnp.int32), jax.random.fold_in(streams_of[3], 1), 0, 1),
    }


diffusion_rate = 0.2

def hat_table(rows, cols, row_shift, col_shift):
    fine_pos = (jnp.arange(rows, dtype=jnp.float32) - row_shift + 0.5) / RATIO - 0.5
    coarse_pos = jnp.arange(cols, dtype=jnp.float32) - col_shift
    return jnp.maximum(0.0, 1.0 - jnp.abs(coarse_pos[None, :] - fine_pos[:, None]))

def smooth_once(padded):
    inner = padded[:, :, 1:-1, 1:-1]
    beside = padded[:, :, 2:, 1:-1] + padded[:, :, :-2, 1:-1] + padded[:, :, 1:-1, 2:] + padded[:, :, 1:-1, :-2]
    return inner + diffusion_rate * (beside - 4.0 * inner)

def diffuse(field):
    for step in range(DSTEPS):
        field = smooth_once(jnp.pad(field, ((0, 0), (0, 0), (1, 1), (1, 1))))
    return field

def forward_increment(ensemble, coarse, fine_x, fine_y):
    scale = 1.0 / math.sqrt(MEMBERS - 1)

    def add_member(total, pair):
        member, weights = pair
        fine = jnp.einsum('xc,lcd,yd->lxy', fine_x, weights, fine_y, precision=lax.Precision.HIGHEST).astype(jnp.bfloat16)
        return (total + member.astype(jnp.float32) * fine.astype(jnp.float32)[None], None)
    total, _ = lax.scan(add_member, jnp.zeros(ensemble.shape[1:], jnp.float32), (ensemble, coarse))
    return total * scale

def adjoint_coarse(ensemble, misfit, fine_x, fine_y):
    scale = 1.0 / math.sqrt(MEMBERS - 1)

    def one_member(member):
        spread = lax.optimization_barrier(jnp.sum(member.astype(jnp.float32) * misfit.astype(jnp.float32), axis=0)) * scale
        return jnp.einsum('xc,lxy,yd->lcd', fine_x, spread, fine_y, precision=lax.Precision.HIGHEST)
    return lax.map(one_member, ensemble)

def reference(ensemble, huber, innovation, sea_mask):
    keep = sea_mask.astype(jnp.float32)
    fine_x = hat_table(NX, NCX, 0, 0)
    fine_y = hat_table(NY, NCY, 0, 0)

    def hessian(field):
        shaped = diffuse(keep * field)
        total = forward_increment(ensemble, shaped, fine_x, fine_y)
        misfit = (huber * total).astype(jnp.bfloat16)
        back = adjoint_coarse(ensemble, misfit, fine_x, fine_y)
        return field + keep * diffuse(back)
    misfit_start = (huber * innovation).astype(jnp.bfloat16)
    gradient = -(keep * diffuse(adjoint_coarse(ensemble, misfit_start, fine_x, fine_y)))
    control = jnp.zeros_like(gradient)
    for step in range(ITERS):
        image = hessian(gradient)
        alpha = jnp.sum(gradient * gradient) / jnp.sum(gradient * image)
        control = control - alpha * gradient
        gradient = gradient - alpha * image
    return (control, gradient)
```

```python
import math

import jax
import jax.numpy as jnp
import numpy as np
from jax import lax
from jax.experimental import pallas as pl
from jax.experimental.pallas import tpu as pltpu
from jax.sharding import PartitionSpec as P


MEMBERS, VARS, LEV = 80, 4, 4
ITERS = 3
GROUPS, PER = 5, 4
OWN_X, OWN_Y = 16, 32
FINE_X, FINE_Y = 64, 128
CHUNK = 16
SX_WEIGHT = (1.0, 2.0, 3.0, 2.0, 1.0)
SY_WEIGHT = (1.0, 2.0, 2.0, 2.0, 1.0)
S_SCALE = 1e-4
MESH = pl.DeviceIdType.MESH
BF, F32 = jnp.bfloat16, jnp.float32


def powers(count, variant):
    where = np.arange(-9, count + 9)
    inside = np.ones(where.shape)
    if variant == 0:
        inside = (where >= 0).astype(float)
    if variant == 2:
        inside = (where < count).astype(float)
    size = where.size
    table = np.eye(size) + 2 * (np.eye(size, k=1) + np.eye(size, k=-1))
    table = inside[:, None] * table * inside[None, :]
    result = [np.diag(inside)]
    for _ in range(4):
        result.append(result[-1] @ table)
    return result


def hat(fine):
    position = (np.arange(fine) + 0.5) / 4 - 0.5
    return lambda c: np.maximum(0.0, 1 - np.abs(c - position))


def window_rows():
    own = [(m, r) for m in range(PER) for r in range(16)]
    halo = [(m, r) for m in range(PER) for r in [*range(-5, 0), *range(16, 21)]]
    return own + halo + [(-1, 0)] * 8


def a_rows():
    return [(m, r) for m in range(PER) for r in range(-1, 17)] + [(-1, 0)] * 8


def b_rows():
    top = [(m, r, 0) for m in range(PER) for r in range(-1, 9)]
    bottom = [(m, r, 0) for m in range(PER) for r in range(7, 17)]
    return top + bottom


def full_rows():
    own = b_rows()
    own = own[:40] + [(m if r > 8 else -1, r, 0) for m, r, _ in own[40:]]
    before = [(m, r - 16, -1) for m in range(PER) for r in range(7, 17)]
    after = [(m, r + 16, 1) for m in range(PER) for r in range(-1, 9)]
    return own + before + after


def window_lanes():
    own = [(l, c) for l in range(LEV) for c in range(32)]
    halo = [(l, c) for l in range(LEV) for c in [*range(-5, 0), *range(32, 37)]]
    return own + halo + [(-1, 0)] * 88


def a_lanes():
    return [(l, c) for l in range(LEV) for c in range(-1, 33)] + [(-1, 0)] * 120


def strip(cells, source):
    return [(l, c, source) for l in range(LEV) for c in cells]


def b_lanes():
    gap = [(-1, 0, 0)]
    first = strip(range(-1, 9), 0) + strip(range(9, 23), 0) + gap * 32
    right, left = strip(range(23, 33), 0), strip(range(-1, 9), 0)
    return first + right + gap * 4 + right + gap * 4 + left


def full_lanes():
    gap = [(-1, 0, 0)]
    first = strip(range(-1, 9), 0) + strip(range(9, 23), 0) + gap * 32
    before, after = strip(range(-9, 1), -1), strip(range(31, 41), 1)
    return first + before + gap * 4 + strip(range(23, 33), 0) + gap * 4 + after


def exists(source, variant):
    return not ((source == -1 and variant == 0) or (source == 1 and variant == 2))


def tables():
    wr, ar, fr = window_rows(), a_rows(), full_rows()
    wl, al, fl = window_lanes(), a_lanes(), full_lanes()
    sxf = np.zeros((3, 5, 80, 128))
    sxb = np.zeros((3, 5, 112, 256))
    for variant in range(3):
        powered = powers(OWN_X, variant)
        for k in range(5):
            for i, (m, r) in enumerate(ar):
                for j, (n, q) in enumerate(wr):
                    if m == n and m >= 0:
                        sxf[variant, k, i, j] = SX_WEIGHT[k] * powered[k][r + 9, q + 9]
            for i, (m, r) in enumerate(wr):
                for j, (n, q, source) in enumerate(fr):
                    if m == n and m >= 0 and exists(source, variant):
                        sxb[variant, k, i, j] = SX_WEIGHT[k] * powered[k][r + 9, q + 9]
    base = np.zeros((3, 5, 64, 128))
    for variant in range(3):
        powered = powers(OWN_Y, variant)
        for k in range(5):
            base[variant, k, 7:57, 7:57] = SY_WEIGHT[k] * powered[4 - k]
    alive = np.zeros((3, 256, 128))
    for variant in range(3):
        for i, (l, c, source) in enumerate(fl):
            alive[variant, i, :] = float(l >= 0 and exists(source, variant))
    pick_w, pick_a, pick_f = (np.zeros((256, 128)) for _ in range(3))
    for table, order in ((pick_w, wl), (pick_a, al), (pick_f, fl)):
        for i, item in enumerate(order):
            if item[0] >= 0:
                table[i, item[1] + 16] = 1
    level = lambda order: np.array([item[0] for item in order])
    same = lambda one, two: ((level(one)[:, None] == level(two)[None, :]) & (level(one)[:, None] >= 0)).astype(float)
    same_wa, same_fw = same(wl, al), same(fl, wl)
    weight_x, weight_y = hat(FINE_X), hat(FINE_Y)
    pxf, pxt = np.zeros((256, 128)), np.zeros((80, 256))
    for j, (m, r) in enumerate(ar):
        if m >= 0:
            pxf[m * 64 : m * 64 + 64, j] = weight_x(r)
    for j, (m, r, _) in enumerate(b_rows()):
        pxt[j, m * 64 : m * 64 + 64] = weight_x(r)
    pyf, pyt = np.zeros((256, 512)), np.zeros((512, 256))
    for j, (l, c) in enumerate(al):
        if l >= 0:
            pyf[j, l * 128 : l * 128 + 128] = weight_y(c)
    for j, (l, c, _) in enumerate(b_lanes()):
        if l >= 0:
            pyt[l * 128 : l * 128 + 128, j] = weight_y(c)
    mask_x, mask_y = np.zeros((80, 16)), np.zeros((32, 256))
    for i, (m, r, _) in enumerate(b_rows()):
        if 0 <= r < 16:
            mask_x[i, r] = 1
    for j, (l, c, _) in enumerate(b_lanes()):
        if l >= 0 and 0 <= c < 32:
            mask_y[c, j] = 1
    home = lambda value, count: -1 if value < 0 else (1 if value >= count else 0)
    take_x, take_y = np.zeros((112, 256)), np.zeros((256, 256))
    for i, (m, r) in enumerate(wr):
        for j, (n, q, source) in enumerate(fr):
            if m == n and m >= 0 and r == q and source == home(r, 16):
                take_x[i, j] = 1
    for j, (l, c) in enumerate(wl):
        for i, (n, q, source) in enumerate(fl):
            if l == n and l >= 0 and c == q and source == home(c, 32):
                take_y[i, j] = 1
    named = dict(
        sxf=sxf, sxb=sxb, base=base, alive=alive, pick_w=pick_w, pick_a=pick_a, pick_f=pick_f, same_wa=same_wa,
        same_fw=same_fw, pxf=pxf, pxt=pxt, pyf=pyf, pyt=pyt, mask_x=mask_x, mask_y=mask_y, take_x=take_x, take_y=take_y,
    )
    return {name: np.asarray(value, np.float32).astype(BF) for name, value in named.items()}


TABLES = tables()
NAMES = tuple(TABLES)
BY_LON, BY_LAT = ("sxf", "sxb"), ("base", "alive")


def dot(a, b):
    return lax.dot_general(a, b, (((1,), (0,)), ((), ())), preferred_element_type=F32)


def dot_nt(a, b):
    return lax.dot_general(a, b, (((1,), (1,)), ((), ())), preferred_element_type=F32)


def kernel(sizes, *refs):
    n_lon, n_lat, n_mem = sizes
    names = ["ens_hbm", "hub_hbm", "inn_hbm", "mask_ref", *(n + "_hbm" for n in NAMES), "out_c", "out_g", "ens", "hub", "inn"]
    names += [*NAMES, "syf", "syb", "win_mask", "grad", "ag", "ctl", "wbuf", "spread", "mis", "rs_own", "rs_send", "rs_recv"]
    names += ["h_send", "h_recv", "sc_send", "sc_m", "sc_y", "sc_x"]
    names += ["in_sem", "ens_sem", "hs_sem", "hr_sem", "rss_sem", "rsr_sem", "ags_sem", "agr_sem", "scs_sem", "scr_sem"]
    r = dict(zip(names, refs, strict=True))
    lon, lat, mem = lax.axis_index("lon"), lax.axis_index("lat"), lax.axis_index("mem")
    scale = 1.0 / math.sqrt(MEMBERS - 1)

    def at(d_lon=0, d_lat=0, d_mem=0):
        return {
            "lon": lax.rem(lon + (d_lon + n_lon), n_lon),
            "lat": lax.rem(lat + (d_lat + n_lat), n_lat),
            "mem": lax.rem(mem + (d_mem + n_mem), n_mem),
        }

    variant_x = jnp.where(lon == 0, 0, jnp.where(lon == n_lon - 1, 2, 1))
    variant_y = jnp.where(lat == 0, 0, jnp.where(lat == n_lat - 1, 2, 1))
    loads = {}
    order = ["base", "alive", "pick_w", "pick_a", "pick_f", "same_wa", "same_fw", "hub", "inn"]
    for i, name in enumerate([*order, *(n for n in NAMES if n not in order)]):
        source = r[name + "_hbm"]
        if name in BY_LON:
            source = source.at[variant_x]
        if name in BY_LAT:
            source = source.at[variant_y]
        loads[name] = pltpu.make_async_copy(source, r[name], r["in_sem"].at[i])
        loads[name].start()
    for g in range(GROUPS):
        part = pl.ds(g * PER, PER)
        pltpu.make_async_copy(r["ens_hbm"].at[part], r["ens"].at[part], r["ens_sem"].at[g]).start()

    barrier = pltpu.get_barrier_semaphore()
    partners = [at(d_mem=d) for d in range(1, n_mem)]
    partners += [at(d_lat=d) for d in range(1, n_lat)]
    partners += [at(d_lon=d) for d in range(1, n_lon)]
    partners += [at(d_lon=dx, d_lat=dy) for dx in (-1, 1) for dy in (-1, 1)]
    for partner in partners:
        pl.semaphore_signal(barrier, inc=1, device_id=partner, device_id_type=MESH)

    lane = lax.broadcasted_iota(jnp.int32, (40, 128), 1)

    for name in order[:7]:
        loads[name].wait()

    @pl.loop(0, 5)
    def _(k):
        base = r["base"][k]
        base = jnp.concatenate([base, jnp.zeros_like(base)], axis=0)
        to_a = dot_nt(base, r["pick_a"][...]).astype(BF)
        to_w = dot_nt(base, r["pick_w"][...]).astype(BF)
        r["syf"][k] = (dot(r["pick_w"][...], to_a).astype(BF) * r["same_wa"][...]).astype(BF)
        spread_f = dot(r["pick_f"][...] * r["alive"][...], to_w).astype(BF)
        r["syb"][k] = (spread_f * r["same_fw"][...]).astype(BF)

    for name in ("hub", "inn"):
        loads[name].wait()

    @pl.loop(0, LEV)
    def _(l):
        for v in range(VARS):
            r["mis"][0, l, v] = (r["hub"][v, l] * r["inn"][v, l]).astype(BF)

    for name in NAMES:
        if name not in order:
            loads[name].wait()
    pl.semaphore_wait(barrier, len(partners))

    def send_strips(e, g, b):
        first, second = b[:, :128], b[:, 128:]
        top, bottom = second[:40], second[40:]
        turned = pltpu.roll(bottom, 64, 1)
        out = r["h_send"].at[e, g]
        out[0] = first[:40].astype(BF)
        out[1] = top.astype(BF)
        out[2] = first[40:].astype(BF)
        out[3] = bottom.astype(BF)
        out[4] = jnp.where(lane < 64, turned, top).astype(BF)
        out[5] = jnp.where(lane < 64, top, turned).astype(BF)
        plan = (
            (4, 1, 5, (0, -1)),
            (5, 1, 4, (0, 1)),
            (4, 1, 9, (-1, -1)),
            (4, 1, 7, (1, -1)),
            (5, 1, 8, (-1, 1)),
            (5, 1, 6, (1, 1)),
            (0, 2, 2, (-1, 0)),
            (2, 2, 0, (1, 0)),
        )
        for source, count, target, (dx, dy) in plan:
            pltpu.make_async_remote_copy(
                src_ref=r["h_send"].at[e, g, pl.ds(source, count)],
                dst_ref=r["h_recv"].at[e, g, pl.ds(target, count)],
                send_sem=r["hs_sem"].at[e],
                recv_sem=r["hr_sem"].at[e, g],
                device_id=at(d_lon=dx, d_lat=dy),
                device_id_type=MESH,
            ).start()

    def adjoint_group(e, g):
        for c in range(FINE_X // CHUNK):
            rows = pl.ds(c * CHUNK, CHUNK)
            for l in range(LEV):
                weights = [r["mis"][e, l, v, rows].astype(F32) for v in range(VARS)]
                for m in range(PER):
                    total = sum(
                        r["ens"][g * PER + m, v, l, rows].astype(F32) * weights[v] for v in range(VARS)
                    )
                    r["spread"][pl.ds(m * 64 + c * CHUNK, CHUNK), l * 128 : l * 128 + 128] = total.astype(BF)
        coarse = dot(r["pxt"][...], r["spread"][...]).astype(BF)
        send_strips(e, g, dot(coarse, r["pyt"][...]) * scale)

    def assembled(e, g):
        pltpu.make_async_copy(r["h_recv"].at[e, g], r["h_recv"].at[e, g], r["hr_sem"].at[e, g]).wait()
        own = [r["h_send"][e, g, i].astype(F32) for i in range(4)]
        got = [r["h_recv"][e, g, i].astype(F32) for i in range(10)]

        def second(before, middle, after, turn):
            if turn:
                before, after = pltpu.roll(before, 64, 1), pltpu.roll(after, 64, 1)
            return jnp.where(lane < 42, before, jnp.where(lane < 86, middle, after))

        first = jnp.concatenate([own[0], own[2], got[0], got[2]], axis=0)
        other = jnp.concatenate(
            [
                second(got[4], own[1], got[5], False),
                second(got[4], own[3], got[5], True),
                second(got[6], got[1], got[7], True),
                second(got[8], got[3], got[9], False),
            ],
            axis=0,
        )
        return jnp.concatenate([first, other], axis=1).astype(BF)

    def smoothed(e, g):
        field = assembled(e, g)
        total = None
        for k in range(5):
            part = dot(r["sxb"][k, :, :160], field).astype(BF)
            part = dot(part, r["syb"][k])
            total = part if total is None else total + part
        return total * r["win_mask"][...]

    mask = r["mask_ref"][...].astype(F32).astype(BF)
    mask_rows = dot(r["mask_x"][...], mask).astype(BF)
    send_strips(0, GROUPS, dot(mask_rows, r["mask_y"][...]))

    @pl.loop(0, GROUPS)
    def _(g):
        part = pl.ds(g * PER, PER)
        pltpu.make_async_copy(r["ens_hbm"].at[part], r["ens"].at[part], r["ens_sem"].at[g]).wait()
        adjoint_group(0, g)

    picked = dot(r["take_x"][:, :160], assembled(0, GROUPS)).astype(BF)
    r["win_mask"][...] = dot(picked, r["take_y"][...]) * S_SCALE

    @pl.loop(0, GROUPS)
    def _(g):
        r["grad"][g] = -smoothed(0, g)
        r["ctl"][g] = jnp.zeros((64, 128), F32)

    row8 = lax.broadcasted_iota(jnp.int32, (8, 128), 0)

    def scalar_send(it, stage, buffer, targets):
        for slot, target in enumerate(targets):
            pltpu.make_async_remote_copy(
                src_ref=r["sc_send"].at[it, stage],
                dst_ref=buffer.at[it, slot],
                send_sem=r["scs_sem"].at[it, stage],
                recv_sem=r["scr_sem"].at[it, stage],
                device_id=target,
                device_id_type=MESH,
            ).start()

    def scalar_sum(it, stage, buffer, count):
        pltpu.make_async_copy(buffer.at[it], buffer.at[it], r["scr_sem"].at[it, stage]).wait()
        total = r["sc_send"][it, stage]
        for slot in range(count):
            total = total + buffer[it, slot]
        return total

    @pl.loop(0, ITERS)
    def _(it):
        squares = jnp.zeros((8, 128), F32)

        def fine_weights(g, squares):
            own = r["grad"][g, :64, :128]
            squares = squares + jnp.sum((own * own).reshape(8, 8, 128), axis=0)
            field = r["grad"][g].astype(BF)
            total = None
            for k in range(5):
                part = dot(r["sxf"][k, :, :112], field).astype(BF)
                part = dot(part, r["syf"][k])
                total = part if total is None else total + part
            coarse = (total * S_SCALE).astype(BF)
            fine = dot(coarse, r["pyf"][...]).astype(BF)
            fine = dot(r["pxf"][:, :80], fine).astype(BF)
            for l in range(LEV):
                r["wbuf"][l, g] = fine[:, l * 128 : l * 128 + 128]
            return squares

        squares = lax.fori_loop(0, GROUPS, fine_weights, squares)

        for step, away in enumerate((2, 1, 3, 0)):
            level = lax.rem(mem + away, n_mem)

            @pl.loop(0, FINE_X // CHUNK)
            def _(c):
                start = pl.multiple_of(c * CHUNK, CHUNK)
                rows = pl.ds(start, CHUNK)
                sums = [jnp.zeros((CHUNK, 128), F32) for _ in range(VARS)]
                for m in range(GROUPS * PER):
                    place = pl.ds(pl.multiple_of((m % PER) * 64 + start, CHUNK), CHUNK)
                    weight = r["wbuf"][level, m // PER, place].astype(F32)
                    for v in range(VARS):
                        sums[v] = sums[v] + r["ens"][m, v, level, rows].astype(F32) * weight
                for v in range(VARS):
                    if away:
                        r["rs_send"][it, step, v, rows] = sums[v].astype(BF)
                    else:
                        r["rs_own"][v, rows] = sums[v]

            if away:
                pltpu.make_async_remote_copy(
                    src_ref=r["rs_send"].at[it, step],
                    dst_ref=r["rs_recv"].at[it, step],
                    send_sem=r["rss_sem"].at[it],
                    recv_sem=r["rsr_sem"].at[it],
                    device_id=at(d_mem=away),
                    device_id_type=MESH,
                ).start()
        pltpu.make_async_copy(r["rs_recv"].at[it], r["rs_recv"].at[it], r["rsr_sem"].at[it]).wait()

        def misfit_rows(c, energy):
            rows = pl.ds(pl.multiple_of(c * CHUNK, CHUNK), CHUNK)
            for v in range(VARS):
                total = r["rs_own"][v, rows]
                for step in range(3):
                    total = total + r["rs_recv"][it, step, v, rows].astype(F32)
                total = total * scale
                rounded = (r["hub"][v, mem, rows] * total).astype(BF)
                r["mis"][it + 1, mem, v, rows] = rounded
                product = rounded.astype(F32) * total
                energy = energy + product[:8] + product[8:]
            return energy

        energy = lax.fori_loop(0, FINE_X // CHUNK, misfit_rows, jnp.zeros((8, 128), F32))
        for away in (2, 1, 3):
            pltpu.make_async_remote_copy(
                src_ref=r["mis"].at[it + 1, mem],
                dst_ref=r["mis"].at[it + 1, mem],
                send_sem=r["ags_sem"].at[it],
                recv_sem=r["agr_sem"].at[it],
                device_id=at(d_mem=away),
                device_id_type=MESH,
            ).start()
        squares = jnp.sum(squares, axis=0, keepdims=True)
        energy = jnp.sum(energy, axis=0, keepdims=True)
        r["sc_send"][it, 0] = jnp.where(row8 == 0, squares, jnp.where(row8 == 1, energy, 0.0))
        scalar_send(it, 0, r["sc_m"], [at(d_mem=d) for d in range(1, n_mem)])
        pltpu.make_async_copy(r["rs_recv"].at[it], r["rs_recv"].at[it], r["agr_sem"].at[it]).wait()
        r["sc_send"][it, 1] = scalar_sum(it, 0, r["sc_m"], n_mem - 1)
        scalar_send(it, 1, r["sc_y"], [at(d_lat=d) for d in range(1, n_lat)])

        @pl.loop(0, GROUPS)
        def _(g):
            adjoint_group(it + 1, g)

        r["sc_send"][it, 2] = scalar_sum(it, 1, r["sc_y"], n_lat - 1)
        scalar_send(it, 2, r["sc_x"], [at(d_lon=d) for d in range(1, n_lon)])

        @pl.loop(0, GROUPS)
        def _(g):
            r["ag"][g] = smoothed(it + 1, g)

        sums = scalar_sum(it, 2, r["sc_x"], n_lon - 1)
        sums = jnp.sum(sums, axis=1, keepdims=True)
        squares, energy = sums[0:1], sums[1:2]
        alpha = squares / (squares + energy)

        @pl.loop(0, GROUPS)
        def _(g):
            gradient = r["grad"][g]
            r["ctl"][g] = r["ctl"][g] - alpha * gradient[:64, :128]
            r["grad"][g] = gradient - alpha * (gradient + r["ag"][g])

    @pl.loop(0, GROUPS)
    def _(g):
        for value, out in ((r["ctl"][g], r["out_c"]), (r["grad"][g, :64, :128], r["out_g"])):
            for l in range(LEV):
                turned = pltpu.roll(value, 128 - 32 * l, 1) if l else value
                for m in range(PER):
                    out[g * PER + m, l] = turned[m * 16 : m * 16 + 16, :32]

    done = lambda ref, sem: pltpu.make_async_copy(ref, ref, sem).wait()
    done(r["h_recv"].at[0], r["hs_sem"].at[0])
    for it in range(ITERS):
        done(r["h_recv"].at[it + 1, pl.ds(0, GROUPS)], r["hs_sem"].at[it + 1])
        done(r["rs_recv"].at[it], r["rss_sem"].at[it])
        done(r["rs_recv"].at[it], r["ags_sem"].at[it])
        for stage, buffer in enumerate(("sc_m", "sc_y", "sc_x")):
            done(r[buffer].at[it], r["scs_sem"].at[it, stage])


def local(sizes, ensemble, huber, innovation, sea_mask):
    n_lon, n_lat, n_mem = sizes
    vmem, dma = pltpu.VMEM, pltpu.SemaphoreType.DMA
    shapes = {n: TABLES[n].shape[1:] if n in BY_LON + BY_LAT else TABLES[n].shape for n in NAMES}
    field = (4, FINE_X, FINE_Y)
    scratch = [
        vmem((MEMBERS // n_mem, VARS, LEV, FINE_X, FINE_Y), BF),
        vmem((VARS, *field), F32),
        vmem((VARS, *field), F32),
        *(vmem(shapes[n], BF) for n in NAMES),
        vmem((5, 256, 256), BF),
        vmem((5, 256, 256), BF),
        vmem((112, 256), F32),
        vmem((GROUPS, 112, 256), F32),
        vmem((GROUPS, 112, 256), F32),
        vmem((GROUPS, 64, 128), F32),
        vmem((LEV, GROUPS, 256, 128), BF),
        vmem((256, 512), BF),
        vmem((ITERS + 1, LEV, *field), BF),
        vmem(field, F32),
        vmem((ITERS, 3, *field), BF),
        vmem((ITERS, 3, *field), BF),
        vmem((ITERS + 1, GROUPS + 1, 6, 40, 128), BF),
        vmem((ITERS + 1, GROUPS + 1, 10, 40, 128), BF),
        vmem((ITERS, 3, 8, 128), F32),
        vmem((ITERS, n_mem - 1, 8, 128), F32),
        vmem((ITERS, n_lat - 1, 8, 128), F32),
        vmem((ITERS, n_lon - 1, 8, 128), F32),
        dma((len(NAMES) + 2,)),
        dma((GROUPS,)),
        dma((ITERS + 1,)),
        dma((ITERS + 1, GROUPS + 1)),
        dma((ITERS,)),
        dma((ITERS,)),
        dma((ITERS,)),
        dma((ITERS,)),
        dma((ITERS, 3)),
        dma((ITERS, 3)),
    ]
    out = jax.ShapeDtypeStruct((MEMBERS // n_mem, LEV, OWN_X, OWN_Y), F32)
    any_space, in_vmem = pl.BlockSpec(memory_space=pl.ANY), pl.BlockSpec(memory_space=pltpu.VMEM)
    return pl.pallas_call(
        lambda *refs: kernel(sizes, *refs),
        out_shape=(out, out),
        in_specs=[any_space, any_space, any_space, in_vmem, *([any_space] * len(NAMES))],
        out_specs=(in_vmem, in_vmem),
        scratch_shapes=scratch,
        name="assimilate",
        compiler_params=pltpu.CompilerParams(collective_id=0, has_side_effects=True, vmem_limit_bytes=60 * 2**20),
    )(ensemble, huber, innovation, sea_mask, *(jnp.asarray(TABLES[n]) for n in NAMES))


def solution(mesh):
    sizes = tuple(mesh.shape[name] for name in ("lon", "lat", "mem"))
    in_specs = (
        P("mem", None, None, "lon", "lat"),
        P(None, None, "lon", "lat"),
        P(None, None, "lon", "lat"),
        P("lon", "lat"),
    )
    out_specs = (P("mem", None, "lon", "lat"), P("mem", None, "lon", "lat"))
    return jax.shard_map(
        lambda *args: local(sizes, *args), mesh=mesh, in_specs=in_specs, out_specs=out_specs, check_vma=False
    )
```

```python
import math
import typing

import jax
import jax.numpy as jnp
import numpy as np
from jax import lax
from jax.experimental import pallas as pl
from jax.experimental.pallas import tpu as pltpu
from jax.sharding import PartitionSpec as P


MEMBERS, VARS, LEV = 80, 4, 4
ITERS = 3
GROUPS, PER = 5, 4
OWN_X, OWN_Y = 16, 32
FINE_X, FINE_Y = 64, 128
CHUNK = 16
CHUNKS = FINE_X // CHUNK
SX_WEIGHT = (1.0, 2.0, 3.0, 2.0, 1.0)
SY_WEIGHT = (1.0, 2.0, 2.0, 2.0, 1.0)
S_SCALE = 1e-4
MESH = pl.DeviceIdType.MESH
BF, F32 = jnp.bfloat16, jnp.float32


def powers(count, variant):
    where = np.arange(-9, count + 9)
    inside = np.ones(where.shape)
    if variant == 0:
        inside = (where >= 0).astype(float)
    if variant == 2:
        inside = (where < count).astype(float)
    size = where.size
    table = np.eye(size) + 2 * (np.eye(size, k=1) + np.eye(size, k=-1))
    table = inside[:, None] * table * inside[None, :]
    result = [np.diag(inside)]
    for _ in range(4):
        result.append(result[-1] @ table)
    return result


def hat(fine):
    position = (np.arange(fine) + 0.5) / 4 - 0.5
    return lambda c: np.maximum(0.0, 1 - np.abs(c - position))


def window_rows():
    own = [(m, r) for m in range(PER) for r in range(16)]
    halo = [(m, r) for m in range(PER) for r in [*range(-5, 0), *range(16, 21)]]
    return own + halo + [(-1, 0)] * 8


def a_rows():
    return [(m, r) for m in range(PER) for r in range(-1, 17)] + [(-1, 0)] * 8


def b_rows():
    top = [(m, r, 0) for m in range(PER) for r in range(-1, 9)]
    bottom = [(m, r, 0) for m in range(PER) for r in range(7, 17)]
    return top + bottom


def full_rows():
    own = b_rows()
    own = own[:40] + [(m if r > 8 else -1, r, 0) for m, r, _ in own[40:]]
    before = [(m, r - 16, -1) for m in range(PER) for r in range(7, 17)]
    after = [(m, r + 16, 1) for m in range(PER) for r in range(-1, 9)]
    return own + before + after


def window_lanes():
    own = [(l, c) for l in range(LEV) for c in range(32)]
    halo = [(l, c) for l in range(LEV) for c in [*range(-5, 0), *range(32, 37)]]
    return own + halo + [(-1, 0)] * 88


def a_lanes():
    return [(l, c) for l in range(LEV) for c in range(-1, 33)] + [(-1, 0)] * 120


def strip(cells, source):
    return [(l, c, source) for l in range(LEV) for c in cells]


def b_lanes():
    gap = [(-1, 0, 0)]
    first = strip(range(-1, 9), 0) + strip(range(9, 23), 0) + gap * 32
    right, left = strip(range(23, 33), 0), strip(range(-1, 9), 0)
    return first + right + gap * 4 + right + gap * 4 + left


def full_lanes():
    gap = [(-1, 0, 0)]
    first = strip(range(-1, 9), 0) + strip(range(9, 23), 0) + gap * 32
    before, after = strip(range(-9, 1), -1), strip(range(31, 41), 1)
    return first + before + gap * 4 + strip(range(23, 33), 0) + gap * 4 + after


def exists(source, variant):
    return not ((source == -1 and variant == 0) or (source == 1 and variant == 2))


def tables():
    wr, ar, fr = window_rows(), a_rows(), full_rows()
    wl, al, fl = window_lanes(), a_lanes(), full_lanes()
    sxf = np.zeros((3, 5, 80, 128))
    sxb = np.zeros((3, 5, 112, 256))
    for variant in range(3):
        powered = powers(OWN_X, variant)
        for k in range(5):
            for i, (m, r) in enumerate(ar):
                for j, (n, q) in enumerate(wr):
                    if m == n and m >= 0:
                        sxf[variant, k, i, j] = SX_WEIGHT[k] * powered[k][r + 9, q + 9]
            for i, (m, r) in enumerate(wr):
                for j, (n, q, source) in enumerate(fr):
                    if m == n and m >= 0 and exists(source, variant):
                        sxb[variant, k, i, j] = SX_WEIGHT[k] * powered[k][r + 9, q + 9]
    base = np.zeros((3, 5, 64, 128))
    for variant in range(3):
        powered = powers(OWN_Y, variant)
        for k in range(5):
            base[variant, k, 7:57, 7:57] = SY_WEIGHT[k] * powered[4 - k]
    alive = np.zeros((3, 256, 128))
    for variant in range(3):
        for i, (l, c, source) in enumerate(fl):
            alive[variant, i, :] = float(l >= 0 and exists(source, variant))
    pick_w, pick_a, pick_f = (np.zeros((256, 128)) for _ in range(3))
    for table, order in ((pick_w, wl), (pick_a, al), (pick_f, fl)):
        for i, item in enumerate(order):
            if item[0] >= 0:
                table[i, item[1] + 16] = 1
    level = lambda order: np.array([item[0] for item in order])
    same = lambda one, two: ((level(one)[:, None] == level(two)[None, :]) & (level(one)[:, None] >= 0)).astype(float)
    same_wa, same_fw = same(wl, al), same(fl, wl)
    weight_x, weight_y = hat(FINE_X), hat(FINE_Y)
    pxf, pxt = np.zeros((256, 128)), np.zeros((80, 256))
    for j, (m, r) in enumerate(ar):
        if m >= 0:
            pxf[m * 64 : m * 64 + 64, j] = weight_x(r)
    for j, (m, r, _) in enumerate(b_rows()):
        pxt[j, m * 64 : m * 64 + 64] = weight_x(r)
    pyf, pyt = np.zeros((256, 512)), np.zeros((512, 256))
    for j, (l, c) in enumerate(al):
        if l >= 0:
            pyf[j, l * 128 : l * 128 + 128] = weight_y(c)
    for j, (l, c, _) in enumerate(b_lanes()):
        if l >= 0:
            pyt[l * 128 : l * 128 + 128, j] = weight_y(c)
    mask_x, mask_y = np.zeros((80, 16)), np.zeros((32, 256))
    for i, (m, r, _) in enumerate(b_rows()):
        if 0 <= r < 16:
            mask_x[i, r] = 1
    for j, (l, c, _) in enumerate(b_lanes()):
        if l >= 0 and 0 <= c < 32:
            mask_y[c, j] = 1
    home = lambda value, count: -1 if value < 0 else (1 if value >= count else 0)
    take_x, take_y = np.zeros((112, 256)), np.zeros((256, 256))
    for i, (m, r) in enumerate(wr):
        for j, (n, q, source) in enumerate(fr):
            if m == n and m >= 0 and r == q and source == home(r, 16):
                take_x[i, j] = 1
    for j, (l, c) in enumerate(wl):
        for i, (n, q, source) in enumerate(fl):
            if l == n and l >= 0 and c == q and source == home(c, 32):
                take_y[i, j] = 1
    named = dict(
        sxf=sxf, sxb=sxb, base=base, alive=alive, pick_w=pick_w, pick_a=pick_a, pick_f=pick_f, same_wa=same_wa,
        same_fw=same_fw, pxf=pxf, pxt=pxt, pyf=pyf, pyt=pyt, mask_x=mask_x, mask_y=mask_y, take_x=take_x, take_y=take_y,
    )
    named.update(sxf=sxf.reshape(3, 400, 128), sxb=sxb.reshape(3, 560, 256))
    return {name: np.asarray(value, np.float32).astype(BF) for name, value in named.items()}


TABLES = tables()
NAMES = tuple(TABLES)
BY_LON, BY_LAT = ("sxf", "sxb"), ("base", "alive")


def dot(a, b):
    return lax.dot_general(a, b, (((1,), (0,)), ((), ())), preferred_element_type=F32)


def dot_nt(a, b):
    return lax.dot_general(a, b, (((1,), (1,)), ((), ())), preferred_element_type=F32)


class Refs(typing.NamedTuple):
    ens_hbm: typing.Any
    hub_hbm: typing.Any
    inn_hbm: typing.Any
    mask_ref: typing.Any
    sxf_hbm: typing.Any
    sxb_hbm: typing.Any
    base_hbm: typing.Any
    alive_hbm: typing.Any
    pick_w_hbm: typing.Any
    pick_a_hbm: typing.Any
    pick_f_hbm: typing.Any
    same_wa_hbm: typing.Any
    same_fw_hbm: typing.Any
    pxf_hbm: typing.Any
    pxt_hbm: typing.Any
    pyf_hbm: typing.Any
    pyt_hbm: typing.Any
    mask_x_hbm: typing.Any
    mask_y_hbm: typing.Any
    take_x_hbm: typing.Any
    take_y_hbm: typing.Any
    out_c: typing.Any
    out_g: typing.Any
    ens: typing.Any
    hub: typing.Any
    inn: typing.Any
    sxf: typing.Any
    sxb: typing.Any
    base: typing.Any
    alive: typing.Any
    pick_w: typing.Any
    pick_a: typing.Any
    pick_f: typing.Any
    same_wa: typing.Any
    same_fw: typing.Any
    pxf: typing.Any
    pxt: typing.Any
    pyf: typing.Any
    pyt: typing.Any
    mask_x: typing.Any
    mask_y: typing.Any
    take_x: typing.Any
    take_y: typing.Any
    syf: typing.Any
    syb: typing.Any
    win_mask: typing.Any
    grad: typing.Any
    ag: typing.Any
    ctl: typing.Any
    u_fwd: typing.Any
    u_back: typing.Any
    coarse: typing.Any
    fine: typing.Any
    wbuf: typing.Any
    spread: typing.Any
    mis: typing.Any
    rs_own: typing.Any
    rs_send: typing.Any
    rs_recv: typing.Any
    h_send: typing.Any
    h_recv: typing.Any
    d_send: typing.Any
    d_recv: typing.Any
    sc_send: typing.Any
    sc_a: typing.Any
    sc_b: typing.Any
    in_sem: typing.Any
    ens_sem: typing.Any
    hs_sem: typing.Any
    hr_sem: typing.Any
    ds_sem: typing.Any
    dr_sem: typing.Any
    rss_sem: typing.Any
    rsr_sem: typing.Any
    ags_sem: typing.Any
    agr_sem: typing.Any
    scs_sem: typing.Any
    scr_sem: typing.Any


def kernel(sizes, *refs):
    n_lon, n_lat, n_mem = sizes
    r = Refs(*refs)
    lon, lat, mem = lax.axis_index("lon"), lax.axis_index("lat"), lax.axis_index("mem")
    scale = 1.0 / math.sqrt(MEMBERS - 1)

    def at(d_lon=0, d_lat=0, d_mem=0):
        return {
            "lon": lax.rem(lon + (d_lon + n_lon), n_lon),
            "lat": lax.rem(lat + (d_lat + n_lat), n_lat),
            "mem": lax.rem(mem + (d_mem + n_mem), n_mem),
        }

    def wait(ref, sem):
        pltpu.make_async_copy(ref, ref, sem).wait()

    def send(source, target, send_sem, recv_sem, device):
        pltpu.make_async_remote_copy(
            src_ref=source, dst_ref=target, send_sem=send_sem, recv_sem=recv_sem, device_id=device, device_id_type=MESH
        ).start()

    variant_x = jnp.where(lon == 0, 0, jnp.where(lon == n_lon - 1, 2, 1))
    variant_y = jnp.where(lat == 0, 0, jnp.where(lat == n_lat - 1, 2, 1))
    loads = {}
    first = ["hub", "inn", "mask_x", "mask_y", "pxt", "pyt"]
    order = [*first, *(n for n in NAMES if n not in first)]

    def load(i):
        name = order[i]
        source = getattr(r, name + "_hbm")
        if name in BY_LON:
            source = source.at[variant_x]
        if name in BY_LAT:
            source = source.at[variant_y]
        loads[name] = pltpu.make_async_copy(source, getattr(r, name), r.in_sem.at[i])
        loads[name].start()

    for i in range(len(first)):
        load(i)
    for g in range(GROUPS):
        part = pl.ds(g * PER, PER)
        pltpu.make_async_copy(r.ens_hbm.at[part], r.ens.at[part], r.ens_sem.at[g]).start()
    for i in range(len(first), len(order)):
        load(i)

    barrier = pltpu.get_barrier_semaphore()
    plane = [at(d_lat=dy, d_mem=dm) for dy in range(n_lat) for dm in range(n_mem) if dy or dm]
    line = [at(d_lon=d) for d in range(1, n_lon)]
    partners = plane + line + [at(d_lon=dx, d_lat=dy) for dx in (-1, 1) for dy in (-1, 1)]
    for partner in partners:
        pl.semaphore_signal(barrier, inc=1, device_id=partner, device_id_type=MESH)

    lane = lax.broadcasted_iota(jnp.int32, (40, 128), 1)
    low = lane[:24] < 64

    for name in first:
        loads[name].wait()

    @pl.loop(0, CHUNKS)
    def _(c):
        rows = pl.ds(pl.multiple_of(c * CHUNK, CHUNK), CHUNK)
        for l in range(LEV):
            for v in range(VARS):
                r.mis[0, c, l, v] = (r.hub[v, l, rows] * r.inn[v, l, rows]).astype(BF)

    with jax.named_scope("w_bar"):
        pl.semaphore_wait(barrier, len(partners))

    def send_strips(e, g, b):
        first, second = b[:, :128], b[:, 128:]
        top, bottom = second[:40], second[40:]
        turned, turned_top = pltpu.roll(bottom, 64, 1), pltpu.roll(top[16:], 64, 1)
        out, corner = r.h_send.at[e, g], r.d_send.at[e, g]
        out[0] = first[:40].astype(BF)
        out[1] = top.astype(BF)
        out[2] = first[40:].astype(BF)
        out[3] = bottom.astype(BF)
        out[4] = jnp.where(lane < 64, turned, top).astype(BF)
        out[5] = jnp.where(lane < 64, top, turned).astype(BF)
        corner[0] = jnp.where(low, turned_top, top[:24]).astype(BF)
        corner[1] = jnp.where(low, top[:24], turned_top).astype(BF)
        corner[2] = jnp.where(low, turned[16:], bottom[:24]).astype(BF)
        corner[3] = jnp.where(low, bottom[:24], turned[16:]).astype(BF)
        strips = ((4, 1, 5, (0, -1)), (5, 1, 4, (0, 1)), (0, 2, 2, (-1, 0)), (2, 2, 0, (1, 0)))
        corners = ((0, 3, (-1, -1)), (1, 2, (-1, 1)), (2, 1, (1, -1)), (3, 0, (1, 1)))
        for source, target, (dx, dy) in corners:
            send(
                r.d_send.at[e, g, source], r.d_recv.at[e, g, target],
                r.ds_sem.at[e], r.dr_sem.at[e, g], at(d_lon=dx, d_lat=dy),
            )
        for source, count, target, (dx, dy) in strips:
            send(
                r.h_send.at[e, g, pl.ds(source, count)], r.h_recv.at[e, g, pl.ds(target, count)],
                r.hs_sem.at[e], r.hr_sem.at[e, g], at(d_lon=dx, d_lat=dy),
            )

    def spread_rows(e, c, g):
        for l in range(LEV):
            weights = [r.mis[e, c, l, v].astype(F32) for v in range(VARS)]
            rows = pl.ds(pl.multiple_of(c * CHUNK, CHUNK), CHUNK)
            for m in range(PER):
                total = sum(r.ens[g * PER + m, v, l, rows].astype(F32) * weights[v] for v in range(VARS))
                place = pl.ds(pl.multiple_of(m * 64 + c * CHUNK, CHUNK), CHUNK)
                r.spread[g, place, l * 128 : l * 128 + 128] = total.astype(BF)

    def coarse_send(e, g):
        rows = dot(r.pxt[...], r.spread[g]).astype(BF)
        send_strips(e, g, dot(rows, r.pyt[...]) * scale)

    def assembled(e, g):
        with jax.named_scope("w_halo"):
            wait(r.h_recv.at[e, g], r.hr_sem.at[e, g])
            wait(r.d_recv.at[e, g], r.dr_sem.at[e, g])
        own = [r.h_send[e, g, i].astype(F32) for i in range(4)]
        got = [r.h_recv[e, g, i].astype(F32) for i in range(6)]
        corner = [r.d_recv[e, g, i].astype(F32) for i in range(4)]
        corner = [jnp.concatenate([d, pltpu.roll(d[8:], 64, 1)], axis=0) for d in corner]

        def second(before, middle, after):
            return jnp.where(lane < 42, before, jnp.where(lane < 86, middle, after))

        first = jnp.concatenate([own[0], own[2], got[0], got[2]], axis=0)
        other = jnp.concatenate(
            [
                second(got[4], own[1], got[5]),
                second(pltpu.roll(got[4], 64, 1), own[3], pltpu.roll(got[5], 64, 1)),
                second(corner[0], got[1], corner[1]),
                second(corner[2], got[3], corner[3]),
            ],
            axis=0,
        )
        return jnp.concatenate([first, other], axis=1).astype(BF)

    def smoothed(e, store):
        for g in range(GROUPS):
            part = dot(r.sxb[:, :160], assembled(e, g))
            for k in range(5):
                r.u_back[k, g * 112 : g * 112 + 112] = part[k * 112 : k * 112 + 112].astype(BF)
        total = dot(r.u_back[0], r.syb[0])
        for k in range(1, 5):
            total = total + dot(r.u_back[k], r.syb[k])
        for g in range(GROUPS):
            store(g, total[g * 112 : g * 112 + 112] * r.win_mask[...])

    mask = r.mask_ref[...].astype(F32).astype(BF)
    mask_rows = dot(r.mask_x[...], mask).astype(BF)
    send_strips(0, GROUPS, dot(mask_rows, r.mask_y[...]))

    @pl.loop(0, GROUPS)
    def _(g):
        part = pl.ds(g * PER, PER)
        with jax.named_scope("w_ens"):
            pltpu.make_async_copy(r.ens_hbm.at[part], r.ens.at[part], r.ens_sem.at[g]).wait()
        with jax.named_scope("adj0"):
            for c in range(CHUNKS):
                spread_rows(0, c, g)
            coarse_send(0, g)

    for name in order:
        if name not in first:
            loads[name].wait()

    @pl.loop(0, 5)
    @jax.named_scope("expand")
    def _(k):
        base = r.base[k]
        base = jnp.concatenate([base, jnp.zeros_like(base)], axis=0)
        to_a = dot_nt(base, r.pick_a[...]).astype(BF)
        to_w = dot_nt(base, r.pick_w[...]).astype(BF)
        r.syf[k] = (dot(r.pick_w[...], to_a).astype(BF) * r.same_wa[...]).astype(BF)
        spread_f = dot(r.pick_f[...] * r.alive[...], to_w).astype(BF)
        r.syb[k] = (spread_f * r.same_fw[...]).astype(BF)

    picked = dot(r.take_x[:, :160], assembled(0, GROUPS)).astype(BF)
    r.win_mask[...] = dot(picked, r.take_y[...]) * S_SCALE

    def store_first(g, value):
        r.grad[g] = -value
        r.ctl[g] = jnp.zeros((64, 128), F32)

    with jax.named_scope("post0"):
        smoothed(0, store_first)

    row8 = lax.broadcasted_iota(jnp.int32, (8, 128), 0)

    def scalar_send(it, stage, buffer, targets):
        for slot, target in enumerate(targets):
            send(
                r.sc_send.at[it, stage], buffer.at[it, slot], r.scs_sem.at[it, stage], r.scr_sem.at[it, stage], target
            )

    def scalar_sum(it, stage, buffer, count):
        with jax.named_scope("w_sc"):
            wait(buffer.at[it], r.scr_sem.at[it, stage])
        total = r.sc_send[it, stage]
        for slot in range(count):
            total = total + buffer[it, slot]
        return total

    @pl.loop(0, ITERS)
    def _(it):
        with jax.named_scope("fine"):
            squares = jnp.zeros((8, 128), F32)
            for g in range(GROUPS):
                own = r.grad[g, :64, :128]
                squares = squares + jnp.sum((own * own).reshape(8, 8, 128), axis=0)
                part = dot(r.sxf[:, :112], r.grad[g].astype(BF))
                for k in range(5):
                    r.u_fwd[k, g * 80 : g * 80 + 80] = part[k * 80 : k * 80 + 80].astype(BF)
            total = dot(r.u_fwd[0], r.syf[0])
            for k in range(1, 5):
                total = total + dot(r.u_fwd[k], r.syf[k])
            r.coarse[...] = (total * S_SCALE).astype(BF)
            r.fine[...] = dot(r.coarse[...], r.pyf[...]).astype(BF)
            for g in range(GROUPS):
                part = dot(r.pxf[:, :80], r.fine[g * 80 : g * 80 + 80]).astype(BF)
                for l in range(LEV):
                    r.wbuf[l, g] = part[:, l * 128 : l * 128 + 128]

        @pl.loop(0, CHUNKS)
        @jax.named_scope("inc")
        def _(c):
            start = pl.multiple_of(c * CHUNK, CHUNK)
            rows = pl.ds(start, CHUNK)
            for step, away in enumerate((2, 1, 3, 0)):
                level = lax.rem(mem + away, n_mem)
                sums = [jnp.zeros((CHUNK, 128), F32) for _ in range(VARS)]
                for m in range(GROUPS * PER):
                    place = pl.ds(pl.multiple_of((m % PER) * 64 + start, CHUNK), CHUNK)
                    weight = r.wbuf[level, m // PER, place].astype(F32)
                    for v in range(VARS):
                        sums[v] = sums[v] + r.ens[m, v, level, rows].astype(F32) * weight
                for v in range(VARS):
                    if away:
                        r.rs_send[it, c, step, v] = sums[v].astype(BF)
                    else:
                        r.rs_own[c, v] = sums[v]
                if away:
                    send(
                        r.rs_send.at[it, c, step], r.rs_recv.at[it, c, step],
                        r.rss_sem.at[it], r.rsr_sem.at[it, c], at(d_mem=away),
                    )

        def misfit_rows(c, energy):
            with jax.named_scope("w_rs"):
                wait(r.rs_recv.at[it, c], r.rsr_sem.at[it, c])
            rows = pl.ds(pl.multiple_of(c * CHUNK, CHUNK), CHUNK)
            for v in range(VARS):
                total = r.rs_own[c, v]
                for step in range(3):
                    total = total + r.rs_recv[it, c, step, v].astype(F32)
                total = total * scale
                rounded = (r.hub[v, mem, rows] * total).astype(BF)
                r.mis[it + 1, c, mem, v] = rounded
                product = rounded.astype(F32) * total
                energy = energy + product[:8] + product[8:]
            for away in (2, 1, 3):
                send(
                    r.mis.at[it + 1, c, mem], r.mis.at[it + 1, c, mem],
                    r.ags_sem.at[it], r.agr_sem.at[it, c], at(d_mem=away),
                )
            return energy

        energy = lax.fori_loop(0, CHUNKS, misfit_rows, jnp.zeros((8, 128), F32))
        squares = jnp.sum(squares, axis=0, keepdims=True)
        energy = jnp.sum(energy, axis=0, keepdims=True)
        r.sc_send[it, 0] = jnp.where(row8 == 0, squares, jnp.where(row8 == 1, energy, 0.0))
        scalar_send(it, 0, r.sc_a, plane)

        @pl.loop(0, CHUNKS - 1)
        def _(c):
            with jax.named_scope("w_ag"):
                wait(r.rs_recv.at[it, c], r.agr_sem.at[it, c])

            with jax.named_scope("adj"):
                @pl.loop(0, GROUPS)
                def _(g):
                    spread_rows(it + 1, c, g)

        with jax.named_scope("w_ag"):
            wait(r.rs_recv.at[it, CHUNKS - 1], r.agr_sem.at[it, CHUNKS - 1])

        with jax.named_scope("adj_send"):
            for g in range(GROUPS):
                spread_rows(it + 1, CHUNKS - 1, g)
                coarse_send(it + 1, g)

        r.sc_send[it, 1] = scalar_sum(it, 0, r.sc_a, len(plane))
        scalar_send(it, 1, r.sc_b, line)

        def store_image(g, value):
            r.ag[g] = value

        with jax.named_scope("post"):
            smoothed(it + 1, store_image)

        sums = scalar_sum(it, 1, r.sc_b, len(line))
        sums = jnp.sum(sums, axis=1, keepdims=True)
        squares, energy = sums[0:1], sums[1:2]
        alpha = squares / (squares + energy)

        with jax.named_scope("upd"):
            for g in range(GROUPS):
                gradient = r.grad[g]
                r.ctl[g] = r.ctl[g] - alpha * gradient[:64, :128]
                r.grad[g] = gradient - alpha * (gradient + r.ag[g])

    for g in range(GROUPS):
        r.out_c[g] = r.ctl[g]
        r.out_g[g] = r.grad[g, :64, :128]

    wait(r.h_recv.at[0], r.hs_sem.at[0])
    wait(r.d_recv.at[0], r.ds_sem.at[0])
    for it in range(ITERS):
        wait(r.h_recv.at[it + 1, pl.ds(0, GROUPS)], r.hs_sem.at[it + 1])
        wait(r.d_recv.at[it + 1, pl.ds(0, GROUPS)], r.ds_sem.at[it + 1])
        wait(r.rs_recv.at[it], r.rss_sem.at[it])
        wait(r.rs_recv.at[it], r.ags_sem.at[it])
        wait(r.sc_a.at[it], r.scs_sem.at[it, 0])
        wait(r.sc_b.at[it], r.scs_sem.at[it, 1])


def unpack(*refs):
    for source, out in (refs[0::2], refs[1::2]):
        for g in range(GROUPS):
            for l in range(LEV):
                turned = pltpu.roll(source[g], 128 - 32 * l, 1) if l else source[g]
                for m in range(PER):
                    out[g * PER + m, l] = turned[m * 16 : m * 16 + 16, :32]


def local(sizes, ensemble, huber, innovation, sea_mask):
    n_lon, n_lat, n_mem = sizes
    vmem, dma = pltpu.VMEM, pltpu.SemaphoreType.DMA
    shapes = {n: TABLES[n].shape[1:] if n in BY_LON + BY_LAT else TABLES[n].shape for n in NAMES}
    field = (VARS, FINE_X, FINE_Y)
    rows = (VARS, CHUNK, FINE_Y)
    times = ITERS + 1
    scratch = [
        vmem((MEMBERS // n_mem, VARS, LEV, FINE_X, FINE_Y), BF),
        vmem((LEV, *field), F32),
        vmem((LEV, *field), F32),
        *(vmem(shapes[n], BF) for n in NAMES),
        vmem((5, 256, 256), BF),
        vmem((5, 256, 256), BF),
        vmem((112, 256), F32),
        vmem((GROUPS, 112, 256), F32),
        vmem((GROUPS, 112, 256), F32),
        vmem((GROUPS, 64, 128), F32),
        vmem((5, GROUPS * 80, 256), BF),
        vmem((5, GROUPS * 112, 256), BF),
        vmem((GROUPS * 80, 256), BF),
        vmem((GROUPS * 80, 512), BF),
        vmem((LEV, GROUPS, 256, 128), BF),
        vmem((GROUPS, 256, 512), BF),
        vmem((times, CHUNKS, LEV, *rows), BF),
        vmem((CHUNKS, *rows), F32),
        vmem((ITERS, CHUNKS, 3, *rows), BF),
        vmem((ITERS, CHUNKS, 3, *rows), BF),
        vmem((times, GROUPS + 1, 6, 40, 128), BF),
        vmem((times, GROUPS + 1, 6, 40, 128), BF),
        vmem((times, GROUPS + 1, 4, 24, 128), BF),
        vmem((times, GROUPS + 1, 4, 24, 128), BF),
        vmem((ITERS, 2, 8, 128), F32),
        vmem((ITERS, n_mem * n_lat - 1, 8, 128), F32),
        vmem((ITERS, n_lon - 1, 8, 128), F32),
        dma((len(NAMES) + 2,)),
        dma((GROUPS,)),
        dma((times,)),
        dma((times, GROUPS + 1)),
        dma((times,)),
        dma((times, GROUPS + 1)),
        dma((ITERS,)),
        dma((ITERS, CHUNKS)),
        dma((ITERS,)),
        dma((ITERS, CHUNKS)),
        dma((ITERS, 2)),
        dma((ITERS, 2)),
    ]
    packed = jax.ShapeDtypeStruct((GROUPS, PER * OWN_X, 128), F32)
    any_space, in_vmem = pl.BlockSpec(memory_space=pl.ANY), pl.BlockSpec(memory_space=pltpu.VMEM)
    control, gradient = pl.pallas_call(
        lambda *refs: kernel(sizes, *refs),
        out_shape=(packed, packed),
        in_specs=[any_space, any_space, any_space, in_vmem, *([any_space] * len(NAMES))],
        out_specs=(in_vmem, in_vmem),
        scratch_shapes=scratch,
        name="assimilate",
        compiler_params=pltpu.CompilerParams(collective_id=0, has_side_effects=True, vmem_limit_bytes=60 * 2**20),
    )(ensemble, huber, innovation, sea_mask, *(jnp.asarray(TABLES[n]) for n in NAMES))
    out = jax.ShapeDtypeStruct((MEMBERS // n_mem, LEV, OWN_X, OWN_Y), F32)
    return pl.pallas_call(
        unpack, out_shape=(out, out), in_specs=[in_vmem] * 2, out_specs=(in_vmem, in_vmem), name="unpack"
    )(control, gradient)


def solution(mesh):
    sizes = tuple(mesh.shape[name] for name in ("lon", "lat", "mem"))
    in_specs = (
        P("mem", None, None, "lon", "lat"),
        P(None, None, "lon", "lat"),
        P(None, None, "lon", "lat"),
        P("lon", "lat"),
    )
    out_specs = (P("mem", None, "lon", "lat"), P("mem", None, "lon", "lat"))
    return jax.shard_map(
        lambda *args: local(sizes, *args), mesh=mesh, in_specs=in_specs, out_specs=out_specs, check_vma=False
    )
```

```python
import math
import typing

import jax
import jax.numpy as jnp
import numpy as np
from jax import lax
from jax.experimental import pallas as pl
from jax.experimental.pallas import tpu as pltpu
from jax.sharding import PartitionSpec as P


MEMBERS, VARS, LEV = 80, 4, 4
ITERS = 3
GROUPS, PER = 5, 4
BATCHES = ((0, 1, 2), (3, 4))
OWN_X, OWN_Y = 16, 32
FINE_X, FINE_Y = 64, 128
CHUNK = 16
CHUNKS = FINE_X // CHUNK
SX_WEIGHT = (1.0, 2.0, 3.0, 2.0, 1.0)
SY_WEIGHT = (1.0, 2.0, 2.0, 2.0, 1.0)
S_SCALE = 1e-4
MESH = pl.DeviceIdType.MESH
BF, F32 = jnp.bfloat16, jnp.float32


def powers(count, variant):
    where = np.arange(-9, count + 9)
    inside = np.ones(where.shape)
    if variant == 0:
        inside = (where >= 0).astype(float)
    if variant == 2:
        inside = (where < count).astype(float)
    size = where.size
    table = np.eye(size) + 2 * (np.eye(size, k=1) + np.eye(size, k=-1))
    table = inside[:, None] * table * inside[None, :]
    result = [np.diag(inside)]
    for _ in range(4):
        result.append(result[-1] @ table)
    return result


def hat(fine):
    position = (np.arange(fine) + 0.5) / 4 - 0.5
    return lambda c: np.maximum(0.0, 1 - np.abs(c - position))


def window_rows():
    own = [(m, r) for m in range(PER) for r in range(16)]
    halo = [(m, r) for m in range(PER) for r in [*range(-5, 0), *range(16, 21)]]
    return own + halo + [(-1, 0)] * 8


def a_rows():
    return [(m, r) for m in range(PER) for r in range(-1, 17)] + [(-1, 0)] * 8


def b_rows():
    top = [(m, r, 0) for m in range(PER) for r in range(-1, 9)]
    bottom = [(m, r, 0) for m in range(PER) for r in range(7, 17)]
    return top + bottom


def full_rows():
    own = b_rows()
    own = own[:40] + [(m if r > 8 else -1, r, 0) for m, r, _ in own[40:]]
    before = [(m, r - 16, -1) for m in range(PER) for r in range(7, 17)]
    after = [(m, r + 16, 1) for m in range(PER) for r in range(-1, 9)]
    return own + before + after


def window_lanes():
    own = [(l, c) for l in range(LEV) for c in range(32)]
    halo = [(l, c) for l in range(LEV) for c in [*range(-5, 0), *range(32, 37)]]
    return own + halo + [(-1, 0)] * 88


def a_lanes():
    return [(l, c) for l in range(LEV) for c in range(-1, 33)] + [(-1, 0)] * 120


def strip(cells, source):
    return [(l, c, source) for l in range(LEV) for c in cells]


def b_lanes():
    gap = [(-1, 0, 0)]
    first = strip(range(-1, 9), 0) + strip(range(9, 23), 0) + gap * 32
    right, left = strip(range(23, 33), 0), strip(range(-1, 9), 0)
    return first + right + gap * 4 + right + gap * 4 + left


def full_lanes():
    gap = [(-1, 0, 0)]
    first = strip(range(-1, 9), 0) + strip(range(9, 23), 0) + gap * 32
    before, after = strip(range(-9, 1), -1), strip(range(31, 41), 1)
    return first + before + gap * 4 + strip(range(23, 33), 0) + gap * 4 + after


def exists(source, variant):
    return not ((source == -1 and variant == 0) or (source == 1 and variant == 2))


def tables():
    wr, ar, fr = window_rows(), a_rows(), full_rows()
    wl, al, fl = window_lanes(), a_lanes(), full_lanes()
    sxf = np.zeros((3, 5, 80, 128))
    sxb = np.zeros((3, 5, 112, 256))
    for variant in range(3):
        powered = powers(OWN_X, variant)
        for k in range(5):
            for i, (m, r) in enumerate(ar):
                for j, (n, q) in enumerate(wr):
                    if m == n and m >= 0:
                        sxf[variant, k, i, j] = SX_WEIGHT[k] * powered[k][r + 9, q + 9]
            for i, (m, r) in enumerate(wr):
                for j, (n, q, source) in enumerate(fr):
                    if m == n and m >= 0 and exists(source, variant):
                        sxb[variant, k, i, j] = SX_WEIGHT[k] * powered[k][r + 9, q + 9]
    base = np.zeros((3, 320, 128))
    for variant in range(3):
        powered = powers(OWN_Y, variant)
        for k in range(5):
            base[variant, k * 64 + 7 : k * 64 + 57, 7:57] = SY_WEIGHT[k] * powered[4 - k]
    alive = np.zeros((3, 256, 128))
    for variant in range(3):
        for i, (l, c, source) in enumerate(fl):
            alive[variant, i, :] = float(l >= 0 and exists(source, variant))
    pick_w, pick_a, pick_f = (np.zeros((256, 128)) for _ in range(3))
    for table, order in ((pick_w, wl), (pick_a, al), (pick_f, fl)):
        for i, item in enumerate(order):
            if item[0] >= 0:
                table[i, item[1] + 16] = 1
    level = lambda order: np.array([item[0] for item in order])
    same = lambda one, two: ((level(one)[:, None] == level(two)[None, :]) & (level(one)[:, None] >= 0)).astype(float)
    same_wa, same_fw = same(wl, al), same(fl, wl)
    weight_x, weight_y = hat(FINE_X), hat(FINE_Y)
    pxf, pxt = np.zeros((256, 128)), np.zeros((80, 256))
    for j, (m, r) in enumerate(ar):
        if m >= 0:
            pxf[m * 64 : m * 64 + 64, j] = weight_x(r)
    for j, (m, r, _) in enumerate(b_rows()):
        pxt[j, m * 64 : m * 64 + 64] = weight_x(r)
    pyf, pyt = np.zeros((256, 512)), np.zeros((512, 256))
    for j, (l, c) in enumerate(al):
        if l >= 0:
            pyf[j, l * 128 : l * 128 + 128] = weight_y(c)
    for j, (l, c, _) in enumerate(b_lanes()):
        if l >= 0:
            pyt[l * 128 : l * 128 + 128, j] = weight_y(c)
    mask_x, mask_y = np.zeros((80, 16)), np.zeros((32, 256))
    for i, (m, r, _) in enumerate(b_rows()):
        if 0 <= r < 16:
            mask_x[i, r] = 1
    for j, (l, c, _) in enumerate(b_lanes()):
        if l >= 0 and 0 <= c < 32:
            mask_y[c, j] = 1
    home = lambda value, count: -1 if value < 0 else (1 if value >= count else 0)
    take_x, take_y = np.zeros((112, 256)), np.zeros((256, 256))
    for i, (m, r) in enumerate(wr):
        for j, (n, q, source) in enumerate(fr):
            if m == n and m >= 0 and r == q and source == home(r, 16):
                take_x[i, j] = 1
    for j, (l, c) in enumerate(wl):
        for i, (n, q, source) in enumerate(fl):
            if l == n and l >= 0 and c == q and source == home(c, 32):
                take_y[i, j] = 1
    named = dict(
        sxf=sxf, sxb=sxb, base=base, alive=alive, pick_w=pick_w, pick_a=pick_a, pick_f=pick_f, same_wa=same_wa,
        same_fw=same_fw, pxf=pxf, pxt=pxt, pyf=pyf, pyt=pyt, mask_x=mask_x, mask_y=mask_y, take_x=take_x, take_y=take_y,
    )
    named.update(sxf=sxf.reshape(3, 400, 128), sxb=sxb.reshape(3, 560, 256))
    return {name: np.asarray(value, np.float32).astype(BF) for name, value in named.items()}


TABLES = tables()
NAMES = tuple(TABLES)
BY_LON, BY_LAT = ("sxf", "sxb"), ("base", "alive")
SPREAD_TABLES = ("base", "alive", "pick_w", "pick_a", "pick_f", "same_wa", "same_fw")


def dot(a, b):
    return lax.dot_general(a, b, (((1,), (0,)), ((), ())), preferred_element_type=F32)


def dot_nt(a, b):
    return lax.dot_general(a, b, (((1,), (1,)), ((), ())), preferred_element_type=F32)


class Refs(typing.NamedTuple):
    ens_hbm: typing.Any
    hub_hbm: typing.Any
    inn_hbm: typing.Any
    mask_hbm: typing.Any
    sxf_hbm: typing.Any
    sxb_hbm: typing.Any
    base_hbm: typing.Any
    alive_hbm: typing.Any
    pick_w_hbm: typing.Any
    pick_a_hbm: typing.Any
    pick_f_hbm: typing.Any
    same_wa_hbm: typing.Any
    same_fw_hbm: typing.Any
    pxf_hbm: typing.Any
    pxt_hbm: typing.Any
    pyf_hbm: typing.Any
    pyt_hbm: typing.Any
    mask_x_hbm: typing.Any
    mask_y_hbm: typing.Any
    take_x_hbm: typing.Any
    take_y_hbm: typing.Any
    out_c: typing.Any
    out_g: typing.Any
    ens: typing.Any
    hub: typing.Any
    inn: typing.Any
    mask: typing.Any
    sxf: typing.Any
    sxb: typing.Any
    base: typing.Any
    alive: typing.Any
    pick_w: typing.Any
    pick_a: typing.Any
    pick_f: typing.Any
    same_wa: typing.Any
    same_fw: typing.Any
    pxf: typing.Any
    pxt: typing.Any
    pyf: typing.Any
    pyt: typing.Any
    mask_x: typing.Any
    mask_y: typing.Any
    take_x: typing.Any
    take_y: typing.Any
    syf: typing.Any
    syb: typing.Any
    win_mask: typing.Any
    grad: typing.Any
    ag: typing.Any
    ctl: typing.Any
    u_fwd: typing.Any
    u_back: typing.Any
    coarse: typing.Any
    fine: typing.Any
    wbuf: typing.Any
    spread: typing.Any
    rows: typing.Any
    mis: typing.Any
    rs_own: typing.Any
    rs_send: typing.Any
    rs_recv: typing.Any
    h_send: typing.Any
    h_recv: typing.Any
    l_send: typing.Any
    l_recv: typing.Any
    d_send: typing.Any
    d_recv: typing.Any
    sc_send: typing.Any
    sc_a: typing.Any
    sc_b: typing.Any
    in_sem: typing.Any
    ens_sem: typing.Any
    hs_sem: typing.Any
    hr_sem: typing.Any
    ls_sem: typing.Any
    lr_sem: typing.Any
    ds_sem: typing.Any
    dr_sem: typing.Any
    rss_sem: typing.Any
    rsr_sem: typing.Any
    ags_sem: typing.Any
    agr_sem: typing.Any
    scs_sem: typing.Any
    scr_sem: typing.Any


def kernel(sizes, *refs):
    n_lon, n_lat, n_mem = sizes
    r = Refs(*refs)
    lon, lat, mem = lax.axis_index("lon"), lax.axis_index("lat"), lax.axis_index("mem")
    scale = 1.0 / math.sqrt(MEMBERS - 1)

    def at(d_lon=0, d_lat=0, d_mem=0):
        return {
            "lon": lax.rem(lon + (d_lon + n_lon), n_lon),
            "lat": lax.rem(lat + (d_lat + n_lat), n_lat),
            "mem": lax.rem(mem + (d_mem + n_mem), n_mem),
        }

    def wait(ref, sem):
        pltpu.make_async_copy(ref, ref, sem).wait()

    def send(source, target, send_sem, recv_sem, device):
        pltpu.make_async_remote_copy(
            src_ref=source, dst_ref=target, send_sem=send_sem, recv_sem=recv_sem, device_id=device, device_id_type=MESH
        ).start()

    variant_x = jnp.where(lon == 0, 0, jnp.where(lon == n_lon - 1, 2, 1))
    variant_y = jnp.where(lat == 0, 0, jnp.where(lat == n_lat - 1, 2, 1))
    loads = {}
    early = [n for n in NAMES if n in SPREAD_TABLES]
    first = ["hub", "inn", "mask", "mask_x", "mask_y", "pxt", "pyt"]
    order = [*early, *first, *(n for n in NAMES if n not in [*early, *first])]

    def load(i):
        name = order[i]
        source = getattr(r, name + "_hbm")
        if name in BY_LON:
            source = source.at[variant_x]
        if name in BY_LAT:
            source = source.at[variant_y]
        loads[name] = pltpu.make_async_copy(source, getattr(r, name), r.in_sem.at[i])
        loads[name].start()

    ready = len(early) + len(first)
    for i in range(ready):
        load(i)
    for g in range(GROUPS):
        part = pl.ds(g * PER, PER)
        pltpu.make_async_copy(r.ens_hbm.at[part], r.ens.at[part], r.ens_sem.at[g]).start()
    for i in range(ready, len(order)):
        load(i)

    barrier = pltpu.get_barrier_semaphore()
    plane = [at(d_lat=dy, d_mem=dm) for dy in range(n_lat) for dm in range(n_mem) if dy or dm]
    line = [at(d_lon=d) for d in range(1, n_lon)]
    partners = plane + line + [at(d_lon=dx, d_lat=dy) for dx in (-1, 1) for dy in (-1, 1)]
    for partner in partners:
        pl.semaphore_signal(barrier, inc=1, device_id=partner, device_id_type=MESH)

    lane = lax.broadcasted_iota(jnp.int32, (40, 128), 1)
    for name in early:
        loads[name].wait()

    with jax.named_scope("expand"):
        to_a = dot_nt(r.base[...], r.pick_a[...]).astype(BF)
        to_w = dot_nt(r.base[...], r.pick_w[...]).astype(BF)
        for k in range(5):
            rows = slice(k * 64, k * 64 + 64)
            r.syf[k] = dot(r.pick_w[:, :64], to_a[rows]).astype(BF) * r.same_wa[...]
            r.syb[k] = dot(r.pick_f[:, :64] * r.alive[:, :64], to_w[rows]).astype(BF) * r.same_fw[...]

    for name in first:
        loads[name].wait()

    @pl.loop(0, CHUNKS)
    def _(c):
        rows = pl.ds(pl.multiple_of(c * CHUNK, CHUNK), CHUNK)
        for l in range(LEV):
            for v in range(VARS):
                r.mis[0, c, l, v] = (r.hub[v, l, rows] * r.inn[v, l, rows]).astype(BF)

    with jax.named_scope("w_bar"):
        pl.semaphore_wait(barrier, len(partners))

    def three(one, two, last, turns):
        one, two, last = (pltpu.roll(x, t, 1) if t else x for x, t in zip((one, two, last), turns))
        at_lane = lane[: one.shape[0]]
        return jnp.where(at_lane < 42, one, jnp.where(at_lane < 86, two, last)).astype(BF)

    def pack_strips(e, g, b):
        first, second = b[:, :128], b[:, 128:]
        out, lats, corner = r.h_send.at[e, g], r.l_send.at[e, g], r.d_send.at[e, g]
        out[0] = first[:40].astype(BF)
        out[1] = second[:40].astype(BF)
        out[2] = first[40:].astype(BF)
        out[3] = second[40:].astype(BF)
        for side, turns in enumerate(((40, 84, 0), (0, 44, 88))):
            lats[side] = three(second[:32], second[24:56], second[48:], turns)
            corner[side] = three(second[:16], second[16:32], second[24:40], turns)
            corner[2 + side] = three(second[40:56], second[56:72], second[64:], turns)

    def send_strips(e, g):
        for source, target, (dx, dy) in ((0, 3, (-1, -1)), (1, 2, (-1, 1)), (2, 1, (1, -1)), (3, 0, (1, 1))):
            send(
                r.d_send.at[e, g, source], r.d_recv.at[e, g, target],
                r.ds_sem.at[e], r.dr_sem.at[e, g], at(d_lon=dx, d_lat=dy),
            )
        for side, dy in ((0, -1), (1, 1)):
            send(
                r.l_send.at[e, g, side], r.l_recv.at[e, g, side], r.ls_sem.at[e], r.lr_sem.at[e, g], at(d_lat=dy)
            )
        for source, target, dx in ((0, 2, -1), (2, 0, 1)):
            send(
                r.h_send.at[e, g, pl.ds(source, 2)], r.h_recv.at[e, g, pl.ds(target, 2)],
                r.hs_sem.at[e], r.hr_sem.at[e, g], at(d_lon=dx),
            )

    def spread_rows(e, c, g):
        for l in range(LEV):
            weights = [r.mis[e, c, l, v].astype(F32) for v in range(VARS)]
            rows = pl.ds(pl.multiple_of(c * CHUNK, CHUNK), CHUNK)
            for m in range(PER):
                total = sum(r.ens[g * PER + m, v, l, rows].astype(F32) * weights[v] for v in range(VARS))
                place = pl.ds(pl.multiple_of(m * 64 + c * CHUNK, CHUNK), CHUNK)
                r.spread[g, place, l * 128 : l * 128 + 128] = total.astype(BF)

    def coarse_rows(e, g):
        r.rows[g * 80 : g * 80 + 80] = dot(r.pxt[...], r.spread[g]).astype(BF)

    def coarse_send(e, groups):
        low, high = groups[0] * 80, groups[-1] * 80 + 80
        total = dot(r.rows[low:high], r.pyt[...]) * scale
        for i, g in enumerate(groups):
            pack_strips(e, g, total[i * 80 : i * 80 + 80])
        for g in groups:
            send_strips(e, g)

    def arrived(e, g):
        with jax.named_scope("w_halo"):
            wait(r.h_recv.at[e, g], r.hr_sem.at[e, g])
            wait(r.l_recv.at[e, g], r.lr_sem.at[e, g])
            wait(r.d_recv.at[e, g], r.dr_sem.at[e, g])

    def assembled(e, g):
        own = [r.h_send[e, g, i].astype(F32) for i in range(4)]
        got = [r.h_recv[e, g, i].astype(F32) for i in range(4)]
        left, right = r.l_recv[e, g, 0].astype(F32), r.l_recv[e, g, 1].astype(F32)
        corner = [r.d_recv[e, g, i].astype(F32) for i in range(4)]
        turn = lambda x, t: pltpu.roll(x, t, 1)

        def second(before, middle, after):
            before, after = jnp.concatenate(before, axis=0), jnp.concatenate(after, axis=0)
            return jnp.where(lane < 42, before, jnp.where(lane < 86, middle, after))

        left_one, left_two = turn(left, 88), turn(left, 44)
        right_two, right_last = turn(right, 84), turn(right, 40)
        from_left = lambda x: [turn(x, 88), turn(x, 44), x[8:]]
        from_right = lambda x: [x, turn(x, 84), turn(x, 40)[8:]]
        first = jnp.concatenate([own[0], own[2], got[0], got[2]], axis=0)
        other = jnp.concatenate(
            [
                second([right, right_two[8:16]], own[1], [left_one, left_two[8:16]]),
                second([right_two[16:], right_last[8:]], own[3], [left_two[16:], left[8:]]),
                second(from_right(corner[0]), got[1], from_left(corner[1])),
                second(from_right(corner[2]), got[3], from_left(corner[3])),
            ],
            axis=0,
        )
        return jnp.concatenate([first, other], axis=1).astype(BF)

    def smoothed(e, store):
        for groups in BATCHES:
            low, high = groups[0] * 112, groups[-1] * 112 + 112
            for g in groups:
                arrived(e, g)
            for g in groups:
                part = dot(r.sxb[:, :160], assembled(e, g))
                for k in range(5):
                    r.u_back[k, g * 112 : g * 112 + 112] = part[k * 112 : k * 112 + 112].astype(BF)
            total = dot(r.u_back[0, low:high], r.syb[0])
            for k in range(1, 5):
                total = total + dot(r.u_back[k, low:high], r.syb[k])
            for i, g in enumerate(groups):
                store(g, total[i * 112 : i * 112 + 112] * r.win_mask[...])

    mask = r.mask[...].astype(F32).astype(BF)
    mask_rows = dot(r.mask_x[...], mask).astype(BF)
    pack_strips(0, GROUPS, dot(mask_rows, r.mask_y[...]))
    send_strips(0, GROUPS)

    for groups in BATCHES:
        for g in groups:
            part = pl.ds(g * PER, PER)
            with jax.named_scope("w_ens"):
                pltpu.make_async_copy(r.ens_hbm.at[part], r.ens.at[part], r.ens_sem.at[g]).wait()

        @pl.loop(groups[0], groups[-1] + 1)
        @jax.named_scope("adj0")
        def _(g):
            for c in range(CHUNKS):
                spread_rows(0, c, g)

        with jax.named_scope("send0"):
            for g in groups:
                coarse_rows(0, g)
            coarse_send(0, groups)

    for name in order[ready:]:
        loads[name].wait()
    arrived(0, GROUPS)

    picked = dot(r.take_x[:, :160], assembled(0, GROUPS)).astype(BF)
    r.win_mask[...] = dot(picked, r.take_y[...]) * S_SCALE

    def store_first(g, value):
        r.grad[g] = -value
        r.ctl[g] = jnp.zeros((64, 128), F32)

    with jax.named_scope("post0"):
        smoothed(0, store_first)

    row8 = lax.broadcasted_iota(jnp.int32, (8, 128), 0)

    def scalar_send(it, stage, buffer, targets):
        for slot, target in enumerate(targets):
            send(
                r.sc_send.at[it, stage], buffer.at[it, slot], r.scs_sem.at[it, stage], r.scr_sem.at[it, stage], target
            )

    def scalar_sum(it, stage, buffer, count):
        with jax.named_scope("w_sc"):
            wait(buffer.at[it], r.scr_sem.at[it, stage])
        total = r.sc_send[it, stage]
        for slot in range(count):
            total = total + buffer[it, slot]
        return total

    @pl.loop(0, ITERS)
    def _(it):
        with jax.named_scope("fine"):
            squares = jnp.zeros((8, 128), F32)
            for g in range(GROUPS):
                own = r.grad[g, :64, :128]
                squares = squares + jnp.sum((own * own).reshape(8, 8, 128), axis=0)
                part = dot(r.sxf[:, :112], r.grad[g].astype(BF))
                for k in range(5):
                    r.u_fwd[k, g * 80 : g * 80 + 80] = part[k * 80 : k * 80 + 80].astype(BF)
            total = dot(r.u_fwd[0], r.syf[0])
            for k in range(1, 5):
                total = total + dot(r.u_fwd[k], r.syf[k])
            r.coarse[...] = (total * S_SCALE).astype(BF)
            r.fine[...] = dot(r.coarse[...], r.pyf[...]).astype(BF)
            for g in range(GROUPS):
                part = dot(r.pxf[:, :80], r.fine[g * 80 : g * 80 + 80]).astype(BF)
                for l in range(LEV):
                    r.wbuf[l, g] = part[:, l * 128 : l * 128 + 128]

        @pl.loop(0, CHUNKS)
        @jax.named_scope("inc")
        def _(c):
            start = pl.multiple_of(c * CHUNK, CHUNK)
            rows = pl.ds(start, CHUNK)
            for step, away in enumerate((2, 1, 3, 0)):
                level = lax.rem(mem + away, n_mem)
                sums = [jnp.zeros((CHUNK, 128), F32) for _ in range(VARS)]
                for m in range(GROUPS * PER):
                    place = pl.ds(pl.multiple_of((m % PER) * 64 + start, CHUNK), CHUNK)
                    weight = r.wbuf[level, m // PER, place].astype(F32)
                    for v in range(VARS):
                        sums[v] = sums[v] + r.ens[m, v, level, rows].astype(F32) * weight
                for v in range(VARS):
                    if away:
                        r.rs_send[it, c, step, v] = sums[v].astype(BF)
                    else:
                        r.rs_own[c, v] = sums[v]
                if away:
                    send(
                        r.rs_send.at[it, c, step], r.rs_recv.at[it, c, step],
                        r.rss_sem.at[it], r.rsr_sem.at[it, c], at(d_mem=away),
                    )

        def misfit_rows(c, energy):
            with jax.named_scope("w_rs"):
                wait(r.rs_recv.at[it, c], r.rsr_sem.at[it, c])
            rows = pl.ds(pl.multiple_of(c * CHUNK, CHUNK), CHUNK)
            for v in range(VARS):
                total = r.rs_own[c, v]
                for step in range(3):
                    total = total + r.rs_recv[it, c, step, v].astype(F32)
                total = total * scale
                rounded = (r.hub[v, mem, rows] * total).astype(BF)
                r.mis[it + 1, c, mem, v] = rounded
                product = rounded.astype(F32) * total
                energy = energy + product[:8] + product[8:]
            for away in (2, 1, 3):
                send(
                    r.mis.at[it + 1, c, mem], r.mis.at[it + 1, c, mem],
                    r.ags_sem.at[it], r.agr_sem.at[it, c], at(d_mem=away),
                )
            return energy

        energy = lax.fori_loop(0, CHUNKS, misfit_rows, jnp.zeros((8, 128), F32))
        squares = jnp.sum(squares, axis=0, keepdims=True)
        energy = jnp.sum(energy, axis=0, keepdims=True)
        r.sc_send[it, 0] = jnp.where(row8 == 0, squares, jnp.where(row8 == 1, energy, 0.0))
        scalar_send(it, 0, r.sc_a, plane)

        @pl.loop(0, CHUNKS - 1)
        def _(c):
            with jax.named_scope("w_ag"):
                wait(r.rs_recv.at[it, c], r.agr_sem.at[it, c])

            with jax.named_scope("adj"):
                @pl.loop(0, GROUPS)
                def _(g):
                    spread_rows(it + 1, c, g)

        with jax.named_scope("w_ag"):
            wait(r.rs_recv.at[it, CHUNKS - 1], r.agr_sem.at[it, CHUNKS - 1])

        with jax.named_scope("adj_send"):
            for groups in BATCHES:
                for g in groups:
                    spread_rows(it + 1, CHUNKS - 1, g)
                for g in groups:
                    coarse_rows(it + 1, g)
                coarse_send(it + 1, groups)

        r.sc_send[it, 1] = scalar_sum(it, 0, r.sc_a, len(plane))
        scalar_send(it, 1, r.sc_b, line)

        def store_image(g, value):
            r.ag[g] = value

        with jax.named_scope("post"):
            smoothed(it + 1, store_image)

        sums = scalar_sum(it, 1, r.sc_b, len(line))
        sums = jnp.sum(sums, axis=1, keepdims=True)
        squares, energy = sums[0:1], sums[1:2]
        alpha = squares / (squares + energy)

        with jax.named_scope("upd"):
            for g in range(GROUPS):
                gradient = r.grad[g]
                r.ctl[g] = r.ctl[g] - alpha * gradient[:64, :128]
                r.grad[g] = gradient - alpha * (gradient + r.ag[g])

    for g in range(GROUPS):
        r.out_c[g] = r.ctl[g]
        r.out_g[g] = r.grad[g, :64, :128]

    wait(r.h_recv.at[0], r.hs_sem.at[0])
    wait(r.l_recv.at[0], r.ls_sem.at[0])
    wait(r.d_recv.at[0], r.ds_sem.at[0])
    for it in range(ITERS):
        wait(r.h_recv.at[it + 1, pl.ds(0, GROUPS)], r.hs_sem.at[it + 1])
        wait(r.l_recv.at[it + 1, pl.ds(0, GROUPS)], r.ls_sem.at[it + 1])
        wait(r.d_recv.at[it + 1, pl.ds(0, GROUPS)], r.ds_sem.at[it + 1])
        wait(r.rs_recv.at[it], r.rss_sem.at[it])
        wait(r.rs_recv.at[it], r.ags_sem.at[it])
        wait(r.sc_a.at[it], r.scs_sem.at[it, 0])
        wait(r.sc_b.at[it], r.scs_sem.at[it, 1])


def unpack(control, gradient, out_c, out_g, packed, spread, in_sem, out_sem):
    sides = ((control, out_c), (gradient, out_g))
    members = [pl.ds(g * PER, PER) for g in range(GROUPS)]
    copies = [[pltpu.make_async_copy(s.at[g], packed.at[i, g], in_sem.at[i, g]) for g in range(GROUPS)] for i, (s, _) in enumerate(sides)]
    backs = [
        [pltpu.make_async_copy(spread.at[i, members[g]], o.at[members[g]], out_sem.at[i, g]) for g in range(GROUPS)]
        for i, (_, o) in enumerate(sides)
    ]
    for i in range(2):
        for g in range(GROUPS):
            copies[i][g].start()
    for i in range(2):
        for g in range(GROUPS):
            copies[i][g].wait()
            for l in range(LEV):
                turned = pltpu.roll(packed[i, g], 128 - 32 * l, 1) if l else packed[i, g]
                for m in range(PER):
                    spread[i, g * PER + m, l] = turned[m * 16 : m * 16 + 16, :32]
            backs[i][g].start()
    for i in range(2):
        for g in range(GROUPS):
            backs[i][g].wait()


def local(sizes, ensemble, huber, innovation, sea_mask):
    n_lon, n_lat, n_mem = sizes
    vmem, dma = pltpu.VMEM, pltpu.SemaphoreType.DMA
    shapes = {n: TABLES[n].shape[1:] if n in BY_LON + BY_LAT else TABLES[n].shape for n in NAMES}
    field = (VARS, FINE_X, FINE_Y)
    rows = (VARS, CHUNK, FINE_Y)
    times = ITERS + 1
    scratch = [
        vmem((MEMBERS // n_mem, VARS, LEV, FINE_X, FINE_Y), BF),
        vmem((LEV, *field), F32),
        vmem((LEV, *field), F32),
        vmem((OWN_X, OWN_Y), jnp.int32),
        *(vmem(shapes[n], BF) for n in NAMES),
        vmem((5, 256, 256), BF),
        vmem((5, 256, 256), BF),
        vmem((112, 256), F32),
        vmem((GROUPS, 112, 256), F32),
        vmem((GROUPS, 112, 256), F32),
        vmem((GROUPS, 64, 128), F32),
        vmem((5, GROUPS * 80, 256), BF),
        vmem((5, GROUPS * 112, 256), BF),
        vmem((GROUPS * 80, 256), BF),
        vmem((GROUPS * 80, 512), BF),
        vmem((LEV, GROUPS, 256, 128), BF),
        vmem((GROUPS, 256, 512), BF),
        vmem((GROUPS * 80, 512), BF),
        vmem((times, CHUNKS, LEV, *rows), BF),
        vmem((CHUNKS, *rows), F32),
        vmem((ITERS, CHUNKS, 3, *rows), BF),
        vmem((ITERS, CHUNKS, 3, *rows), BF),
        vmem((times, GROUPS + 1, 4, 40, 128), BF),
        vmem((times, GROUPS + 1, 4, 40, 128), BF),
        vmem((times, GROUPS + 1, 2, 32, 128), BF),
        vmem((times, GROUPS + 1, 2, 32, 128), BF),
        vmem((times, GROUPS + 1, 4, 16, 128), BF),
        vmem((times, GROUPS + 1, 4, 16, 128), BF),
        vmem((ITERS, 2, 8, 128), F32),
        vmem((ITERS, n_mem * n_lat - 1, 8, 128), F32),
        vmem((ITERS, n_lon - 1, 8, 128), F32),
        dma((len(NAMES) + 3,)),
        dma((GROUPS,)),
        dma((times,)),
        dma((times, GROUPS + 1)),
        dma((times,)),
        dma((times, GROUPS + 1)),
        dma((times,)),
        dma((times, GROUPS + 1)),
        dma((ITERS,)),
        dma((ITERS, CHUNKS)),
        dma((ITERS,)),
        dma((ITERS, CHUNKS)),
        dma((ITERS, 2)),
        dma((ITERS, 2)),
    ]
    packed = jax.ShapeDtypeStruct((GROUPS, PER * OWN_X, 128), F32)
    any_space, in_vmem = pl.BlockSpec(memory_space=pl.ANY), pl.BlockSpec(memory_space=pltpu.VMEM)
    control, gradient = pl.pallas_call(
        lambda *refs: kernel(sizes, *refs),
        out_shape=(packed, packed),
        in_specs=[any_space] * (4 + len(NAMES)),
        out_specs=(in_vmem, in_vmem),
        scratch_shapes=scratch,
        name="assimilate",
        compiler_params=pltpu.CompilerParams(collective_id=0, has_side_effects=True, vmem_limit_bytes=60 * 2**20),
    )(ensemble, huber, innovation, sea_mask, *(jnp.asarray(TABLES[n]) for n in NAMES))
    out = jax.ShapeDtypeStruct((MEMBERS // n_mem, LEV, OWN_X, OWN_Y), F32)
    return pl.pallas_call(
        unpack,
        out_shape=(out, out),
        in_specs=[any_space] * 2,
        out_specs=(any_space, any_space),
        scratch_shapes=[
            vmem((2, *packed.shape), F32),
            vmem((2, *out.shape), F32),
            dma((2, GROUPS)),
            dma((2, GROUPS)),
        ],
        name="unpack",
    )(control, gradient)


def solution(mesh):
    sizes = tuple(mesh.shape[name] for name in ("lon", "lat", "mem"))
    in_specs = (
        P("mem", None, None, "lon", "lat"),
        P(None, None, "lon", "lat"),
        P(None, None, "lon", "lat"),
        P("lon", "lat"),
    )
    out_specs = (P("mem", None, "lon", "lat"), P("mem", None, "lon", "lat"))
    return jax.shard_map(
        lambda *args: local(sizes, *args), mesh=mesh, in_specs=in_specs, out_specs=out_specs, check_vma=False
    )
```

```python
import math
import typing

import jax
import jax.numpy as jnp
import numpy as np
from jax import lax
from jax.experimental import pallas as pl
from jax.experimental.pallas import tpu as pltpu
from jax.sharding import PartitionSpec as P


MEMBERS, VARS, LEV = 80, 4, 4
ITERS = 3
GROUPS, PER = 5, 4
BATCHES = ((0, 1), (2, 3, 4))
OWN_X, OWN_Y = 16, 32
FINE_X, FINE_Y = 64, 128
CHUNK = 16
CHUNKS = FINE_X // CHUNK
SX_WEIGHT = (1.0, 2.0, 3.0, 2.0, 1.0)
SY_WEIGHT = (1.0, 2.0, 2.0, 2.0, 1.0)
S_SCALE = 1e-4
MESH = pl.DeviceIdType.MESH
BF, F32 = jnp.bfloat16, jnp.float32


def powers(count, variant):
    where = np.arange(-9, count + 9)
    inside = np.ones(where.shape)
    if variant == 0:
        inside = (where >= 0).astype(float)
    if variant == 2:
        inside = (where < count).astype(float)
    size = where.size
    table = np.eye(size) + 2 * (np.eye(size, k=1) + np.eye(size, k=-1))
    table = inside[:, None] * table * inside[None, :]
    result = [np.diag(inside)]
    for _ in range(4):
        result.append(result[-1] @ table)
    return result


def hat(fine):
    position = (np.arange(fine) + 0.5) / 4 - 0.5
    return lambda c: np.maximum(0.0, 1 - np.abs(c - position))


def window_rows():
    own = [(m, r) for m in range(PER) for r in range(16)]
    halo = [(m, r) for m in range(PER) for r in [*range(-5, 0), *range(16, 21)]]
    return own + halo + [(-1, 0)] * 8


def a_rows():
    return [(m, r) for m in range(PER) for r in range(-1, 17)] + [(-1, 0)] * 8


def b_rows():
    top = [(m, r, 0) for m in range(PER) for r in range(-1, 9)]
    bottom = [(m, r, 0) for m in range(PER) for r in range(7, 17)]
    return top + bottom


def full_rows():
    own = b_rows()
    own = own[:40] + [(m if r > 8 else -1, r, 0) for m, r, _ in own[40:]]
    before = [(m, r - 16, -1) for m in range(PER) for r in range(7, 17)]
    after = [(m, r + 16, 1) for m in range(PER) for r in range(-1, 9)]
    return own + before + after


def window_lanes():
    own = [(l, c) for l in range(LEV) for c in range(32)]
    halo = [(l, c) for l in range(LEV) for c in [*range(-5, 0), *range(32, 37)]]
    return own + halo + [(-1, 0)] * 88


def a_lanes():
    return [(l, c) for l in range(LEV) for c in range(-1, 33)] + [(-1, 0)] * 120


def strip(cells, source):
    return [(l, c, source) for l in range(LEV) for c in cells]


def b_lanes():
    gap = [(-1, 0, 0)]
    first = strip(range(-1, 9), 0) + strip(range(9, 23), 0) + gap * 32
    right, left = strip(range(23, 33), 0), strip(range(-1, 9), 0)
    return first + right + gap * 4 + right + gap * 4 + left


def full_lanes():
    gap = [(-1, 0, 0)]
    first = strip(range(-1, 9), 0) + strip(range(9, 23), 0) + gap * 32
    before, after = strip(range(-9, 1), -1), strip(range(31, 41), 1)
    return first + before + gap * 4 + strip(range(23, 33), 0) + gap * 4 + after


def exists(source, variant):
    return not ((source == -1 and variant == 0) or (source == 1 and variant == 2))


def tables():
    wr, ar, fr = window_rows(), a_rows(), full_rows()
    wl, al, fl = window_lanes(), a_lanes(), full_lanes()
    sxf = np.zeros((3, 5, 80, 128))
    sxb = np.zeros((3, 5, 112, 256))
    for variant in range(3):
        powered = powers(OWN_X, variant)
        for k in range(5):
            for i, (m, r) in enumerate(ar):
                for j, (n, q) in enumerate(wr):
                    if m == n and m >= 0:
                        sxf[variant, k, i, j] = SX_WEIGHT[k] * powered[k][r + 9, q + 9]
            for i, (m, r) in enumerate(wr):
                for j, (n, q, source) in enumerate(fr):
                    if m == n and m >= 0 and exists(source, variant):
                        sxb[variant, k, i, j] = SX_WEIGHT[k] * powered[k][r + 9, q + 9]
    base = np.zeros((3, 320, 128))
    for variant in range(3):
        powered = powers(OWN_Y, variant)
        for k in range(5):
            base[variant, k * 64 + 7 : k * 64 + 57, 7:57] = SY_WEIGHT[k] * powered[4 - k]
    alive = np.zeros((3, 256, 128))
    for variant in range(3):
        for i, (l, c, source) in enumerate(fl):
            alive[variant, i, :] = float(l >= 0 and exists(source, variant))
    pick_w, pick_a, pick_f = (np.zeros((256, 128)) for _ in range(3))
    for table, order in ((pick_w, wl), (pick_a, al), (pick_f, fl)):
        for i, item in enumerate(order):
            if item[0] >= 0:
                table[i, item[1] + 16] = 1
    level = lambda order: np.array([item[0] for item in order])
    same = lambda one, two: ((level(one)[:, None] == level(two)[None, :]) & (level(one)[:, None] >= 0)).astype(float)
    same_wa, same_fw = same(wl, al), same(fl, wl)
    weight_x, weight_y = hat(FINE_X), hat(FINE_Y)
    pxf, pxt = np.zeros((4, 4, 16, 128)), np.zeros((80, 256))
    for j, (m, r) in enumerate(ar):
        if m >= 0:
            pxf[:, m, :, j] = weight_x(r).reshape(4, 16)
    for j, (m, r, _) in enumerate(b_rows()):
        pxt[j, m * 64 : m * 64 + 64] = weight_x(r)
    pyf, pyt = np.zeros((256, 512)), np.zeros((512, 256))
    for j, (l, c) in enumerate(al):
        if l >= 0:
            pyf[j, l * 128 : l * 128 + 128] = weight_y(c)
    for j, (l, c, _) in enumerate(b_lanes()):
        if l >= 0:
            pyt[l * 128 : l * 128 + 128, j] = weight_y(c)
    mask_x, mask_y = np.zeros((80, 16)), np.zeros((32, 256))
    for i, (m, r, _) in enumerate(b_rows()):
        if 0 <= r < 16:
            mask_x[i, r] = 1
    for j, (l, c, _) in enumerate(b_lanes()):
        if l >= 0 and 0 <= c < 32:
            mask_y[c, j] = 1
    home = lambda value, count: -1 if value < 0 else (1 if value >= count else 0)
    take_x, take_y = np.zeros((112, 256)), np.zeros((256, 256))
    for i, (m, r) in enumerate(wr):
        for j, (n, q, source) in enumerate(fr):
            if m == n and m >= 0 and r == q and source == home(r, 16):
                take_x[i, j] = 1
    for j, (l, c) in enumerate(wl):
        for i, (n, q, source) in enumerate(fl):
            if l == n and l >= 0 and c == q and source == home(c, 32):
                take_y[i, j] = 1
    named = dict(
        sxf=sxf, sxb=sxb, base=base, alive=alive, pick_w=pick_w, pick_a=pick_a, pick_f=pick_f, same_wa=same_wa,
        same_fw=same_fw, pxf=pxf, pxt=pxt, pyf=pyf, pyt=pyt, mask_x=mask_x, mask_y=mask_y, take_x=take_x, take_y=take_y,
    )
    named.update(pxf=pxf.reshape(4, 64, 128), sxf=sxf.reshape(3, 400, 128), sxb=sxb.reshape(3, 560, 256))
    return {name: np.asarray(value, np.float32).astype(BF) for name, value in named.items()}


TABLES = tables()
NAMES = tuple(TABLES)
BY_LON, BY_LAT = ("sxf", "sxb"), ("base", "alive")


def dot(a, b):
    return lax.dot_general(a, b, (((1,), (0,)), ((), ())), preferred_element_type=F32)


def summed(rows, tables, low, high):
    middle = low + (high - low) // 32 * 16
    halves = []
    for start, stop in ((low, middle), (middle, high)):
        total = dot(rows[0, start:stop], tables[0])
        for k in range(1, 5):
            total = total + dot(rows[k, start:stop], tables[k])
        halves.append(total)
    return jnp.concatenate(halves, axis=0)


def dot_nt(a, b):
    return lax.dot_general(a, b, (((1,), (1,)), ((), ())), preferred_element_type=F32)


class Refs(typing.NamedTuple):
    ens_hbm: typing.Any
    hub_hbm: typing.Any
    inn_hbm: typing.Any
    mask_hbm: typing.Any
    sxf_hbm: typing.Any
    sxb_hbm: typing.Any
    base_hbm: typing.Any
    alive_hbm: typing.Any
    pick_w_hbm: typing.Any
    pick_a_hbm: typing.Any
    pick_f_hbm: typing.Any
    same_wa_hbm: typing.Any
    same_fw_hbm: typing.Any
    pxf_hbm: typing.Any
    pxt_hbm: typing.Any
    pyf_hbm: typing.Any
    pyt_hbm: typing.Any
    mask_x_hbm: typing.Any
    mask_y_hbm: typing.Any
    take_x_hbm: typing.Any
    take_y_hbm: typing.Any
    out_c: typing.Any
    out_g: typing.Any
    ens: typing.Any
    hub: typing.Any
    inn: typing.Any
    mask: typing.Any
    sxf: typing.Any
    sxb: typing.Any
    base: typing.Any
    alive: typing.Any
    pick_w: typing.Any
    pick_a: typing.Any
    pick_f: typing.Any
    same_wa: typing.Any
    same_fw: typing.Any
    pxf: typing.Any
    pxt: typing.Any
    pyf: typing.Any
    pyt: typing.Any
    mask_x: typing.Any
    mask_y: typing.Any
    take_x: typing.Any
    take_y: typing.Any
    syf: typing.Any
    syb: typing.Any
    win_mask: typing.Any
    grad: typing.Any
    ag: typing.Any
    ctl: typing.Any
    u_fwd: typing.Any
    u_back: typing.Any
    coarse: typing.Any
    fine: typing.Any
    wbuf: typing.Any
    spread: typing.Any
    rows: typing.Any
    mis: typing.Any
    rs_own: typing.Any
    rs_send: typing.Any
    rs_recv: typing.Any
    h_send: typing.Any
    h_recv: typing.Any
    l_send: typing.Any
    l_recv: typing.Any
    d_send: typing.Any
    d_recv: typing.Any
    sc_send: typing.Any
    sc_a: typing.Any
    sc_b: typing.Any
    in_sem: typing.Any
    ens_sem: typing.Any
    hs_sem: typing.Any
    hr_sem: typing.Any
    ls_sem: typing.Any
    lr_sem: typing.Any
    ds_sem: typing.Any
    dr_sem: typing.Any
    rss_sem: typing.Any
    rsr_sem: typing.Any
    ags_sem: typing.Any
    agr_sem: typing.Any
    scs_sem: typing.Any
    scr_sem: typing.Any


def kernel(sizes, *refs):
    n_lon, n_lat, n_mem = sizes
    r = Refs(*refs)
    lon, lat, mem = lax.axis_index("lon"), lax.axis_index("lat"), lax.axis_index("mem")
    scale = 1.0 / math.sqrt(MEMBERS - 1)

    def at(d_lon=0, d_lat=0, d_mem=0):
        return {
            "lon": lax.rem(lon + (d_lon + n_lon), n_lon),
            "lat": lax.rem(lat + (d_lat + n_lat), n_lat),
            "mem": lax.rem(mem + (d_mem + n_mem), n_mem),
        }

    def wait(ref, sem):
        pltpu.make_async_copy(ref, ref, sem).wait()

    def send(source, target, send_sem, recv_sem, device):
        pltpu.make_async_remote_copy(
            src_ref=source, dst_ref=target, send_sem=send_sem, recv_sem=recv_sem, device_id=device, device_id_type=MESH
        ).start()

    variant_x = jnp.where(lon == 0, 0, jnp.where(lon == n_lon - 1, 2, 1))
    variant_y = jnp.where(lat == 0, 0, jnp.where(lat == n_lat - 1, 2, 1))
    loads = {}
    first = ["hub", "inn", "mask", "mask_x", "mask_y", "pxt", "pyt"]
    order = [*first, *(n for n in NAMES if n not in first)]

    def load(i):
        name = order[i]
        source = getattr(r, name + "_hbm")
        if name in BY_LON:
            source = source.at[variant_x]
        if name in BY_LAT:
            source = source.at[variant_y]
        loads[name] = pltpu.make_async_copy(source, getattr(r, name), r.in_sem.at[i])
        loads[name].start()

    ready = len(first)
    for i in range(ready):
        load(i)
    for g in range(GROUPS):
        part = pl.ds(g * PER, PER)
        pltpu.make_async_copy(r.ens_hbm.at[part], r.ens.at[part], r.ens_sem.at[g]).start()
    for i in range(ready, len(order)):
        load(i)

    barrier = pltpu.get_barrier_semaphore()
    plane = [at(d_lat=dy, d_mem=dm) for dy in range(n_lat) for dm in range(n_mem) if dy or dm]
    line = [at(d_lon=d) for d in range(1, n_lon)]
    partners = plane + line + [at(d_lon=dx, d_lat=dy) for dx in (-1, 1) for dy in (-1, 1)]
    for partner in partners:
        pl.semaphore_signal(barrier, inc=1, device_id=partner, device_id_type=MESH)

    lane = lax.broadcasted_iota(jnp.int32, (40, 128), 1)
    for name in first:
        loads[name].wait()

    @pl.loop(0, CHUNKS)
    def _(c):
        rows = pl.ds(pl.multiple_of(c * CHUNK, CHUNK), CHUNK)
        for l in range(LEV):
            for v in range(VARS):
                r.mis[0, c, l, v] = (r.hub[v, l, rows] * r.inn[v, l, rows]).astype(BF)

    with jax.named_scope("w_bar"):
        pl.semaphore_wait(barrier, len(partners))

    def three(one, two, last, turns):
        one, two, last = (pltpu.roll(x, t, 1) if t else x for x, t in zip((one, two, last), turns))
        at_lane = lane[: one.shape[0]]
        return jnp.where(at_lane < 42, one, jnp.where(at_lane < 86, two, last)).astype(BF)

    def pack_strips(e, g, b):
        first, second = b[:, :128], b[:, 128:]
        out, lats, corner = r.h_send.at[e, g], r.l_send.at[e, g], r.d_send.at[e, g]
        out[0] = first[:40].astype(BF)
        out[1] = second[:40].astype(BF)
        out[2] = first[40:].astype(BF)
        out[3] = second[40:].astype(BF)
        for side, turns in enumerate(((40, 84, 0), (0, 44, 88))):
            lats[side] = three(second[:32], second[24:56], second[48:], turns)
            corner[side] = three(second[:16], second[16:32], second[24:40], turns)
            corner[2 + side] = three(second[40:56], second[56:72], second[64:], turns)

    def send_strips(e, g):
        for source, target, (dx, dy) in ((0, 3, (-1, -1)), (1, 2, (-1, 1)), (2, 1, (1, -1)), (3, 0, (1, 1))):
            send(
                r.d_send.at[e, g, source], r.d_recv.at[e, g, target],
                r.ds_sem.at[e], r.dr_sem.at[e, g], at(d_lon=dx, d_lat=dy),
            )
        for side, dy in ((0, -1), (1, 1)):
            send(
                r.l_send.at[e, g, side], r.l_recv.at[e, g, side], r.ls_sem.at[e], r.lr_sem.at[e, g], at(d_lat=dy)
            )
        for source, target, dx in ((0, 2, -1), (2, 0, 1)):
            send(
                r.h_send.at[e, g, pl.ds(source, 2)], r.h_recv.at[e, g, pl.ds(target, 2)],
                r.hs_sem.at[e], r.hr_sem.at[e, g], at(d_lon=dx),
            )

    def spread_rows(e, c, g):
        for l in range(LEV):
            weights = [r.mis[e, c, l, v].astype(F32) for v in range(VARS)]
            rows = pl.ds(pl.multiple_of(c * CHUNK, CHUNK), CHUNK)
            for m in range(PER):
                total = sum(r.ens[g * PER + m, v, l, rows].astype(F32) * weights[v] for v in range(VARS))
                place = pl.ds(pl.multiple_of(m * 64 + c * CHUNK, CHUNK), CHUNK)
                r.spread[g, place, l * 128 : l * 128 + 128] = total.astype(BF)

    def coarse_rows(e, g):
        r.rows[g * 80 : g * 80 + 80] = dot(r.pxt[...], r.spread[g]).astype(BF)

    def coarse_send(e, groups):
        low, high = groups[0] * 80, groups[-1] * 80 + 80
        total = dot(r.rows[low:high], r.pyt[...]) * scale
        for i, g in enumerate(groups):
            pack_strips(e, g, total[i * 80 : i * 80 + 80])
        for g in groups:
            send_strips(e, g)

    def arrived(e, g):
        with jax.named_scope("w_halo"):
            wait(r.h_recv.at[e, g], r.hr_sem.at[e, g])
            wait(r.l_recv.at[e, g], r.lr_sem.at[e, g])
            wait(r.d_recv.at[e, g], r.dr_sem.at[e, g])

    def assembled(e, g):
        own = [r.h_send[e, g, i].astype(F32) for i in range(4)]
        got = [r.h_recv[e, g, i].astype(F32) for i in range(4)]
        left, right = r.l_recv[e, g, 0].astype(F32), r.l_recv[e, g, 1].astype(F32)
        corner = [r.d_recv[e, g, i].astype(F32) for i in range(4)]
        turn = lambda x, t: pltpu.roll(x, t, 1)

        def second(before, middle, after):
            before, after = jnp.concatenate(before, axis=0), jnp.concatenate(after, axis=0)
            return jnp.where(lane < 42, before, jnp.where(lane < 86, middle, after))

        left_one, left_two = turn(left, 88), turn(left, 44)
        right_two, right_last = turn(right, 84), turn(right, 40)
        from_left = lambda x: [turn(x, 88), turn(x, 44), x[8:]]
        from_right = lambda x: [x, turn(x, 84), turn(x, 40)[8:]]
        first = jnp.concatenate([own[0], own[2], got[0], got[2]], axis=0)
        other = jnp.concatenate(
            [
                second([right, right_two[8:16]], own[1], [left_one, left_two[8:16]]),
                second([right_two[16:], right_last[8:]], own[3], [left_two[16:], left[8:]]),
                second(from_right(corner[0]), got[1], from_left(corner[1])),
                second(from_right(corner[2]), got[3], from_left(corner[3])),
            ],
            axis=0,
        )
        return jnp.concatenate([first, other], axis=1).astype(BF)

    def smoothed(e, store):
        for groups in BATCHES:
            low, high = groups[0] * 112, groups[-1] * 112 + 112
            for g in groups:
                arrived(e, g)
            for g in groups:
                part = dot(r.sxb[:, :160], assembled(e, g))
                for k in range(5):
                    r.u_back[k, g * 112 : g * 112 + 112] = part[k * 112 : k * 112 + 112].astype(BF)
            total = summed(r.u_back, r.syb, low, high)
            for i, g in enumerate(groups):
                store(g, total[i * 112 : i * 112 + 112] * r.win_mask[...])

    mask = r.mask[...].astype(F32).astype(BF)
    mask_rows = dot(r.mask_x[...], mask).astype(BF)
    pack_strips(0, GROUPS, dot(mask_rows, r.mask_y[...]))
    send_strips(0, GROUPS)

    for groups in BATCHES:
        for g in groups:
            part = pl.ds(g * PER, PER)
            with jax.named_scope("w_ens"):
                pltpu.make_async_copy(r.ens_hbm.at[part], r.ens.at[part], r.ens_sem.at[g]).wait()

        @pl.loop(groups[0], groups[-1] + 1)
        @jax.named_scope("adj0")
        def _(g):
            for c in range(CHUNKS):
                spread_rows(0, c, g)

        with jax.named_scope("send0"):
            for g in groups:
                coarse_rows(0, g)
            coarse_send(0, groups)

    for name in order[ready:]:
        loads[name].wait()

    with jax.named_scope("expand"):
        to_a = dot_nt(r.base[...], r.pick_a[...]).astype(BF)
        to_w = dot_nt(r.base[...], r.pick_w[...]).astype(BF)
        for k in range(5):
            rows = slice(k * 64, k * 64 + 64)
            r.syf[k] = dot(r.pick_w[:, :64], to_a[rows]).astype(BF) * r.same_wa[...]
            r.syb[k] = dot(r.pick_f[:, :64] * r.alive[:, :64], to_w[rows]).astype(BF) * r.same_fw[...]

    arrived(0, GROUPS)

    picked = dot(r.take_x[:, :160], assembled(0, GROUPS)).astype(BF)
    r.win_mask[...] = dot(picked, r.take_y[...]) * S_SCALE

    def store_first(g, value):
        r.grad[g] = -value
        r.ctl[g] = jnp.zeros((64, 128), F32)

    with jax.named_scope("post0"):
        smoothed(0, store_first)

    row8 = lax.broadcasted_iota(jnp.int32, (8, 128), 0)

    def scalar_send(it, stage, buffer, targets):
        for slot, target in enumerate(targets):
            send(
                r.sc_send.at[it, stage], buffer.at[it, slot], r.scs_sem.at[it, stage], r.scr_sem.at[it, stage], target
            )

    def scalar_sum(it, stage, buffer, count):
        with jax.named_scope("w_sc"):
            wait(buffer.at[it], r.scr_sem.at[it, stage])
        total = r.sc_send[it, stage]
        for slot in range(count):
            total = total + buffer[it, slot]
        return total

    @pl.loop(0, ITERS)
    def _(it):
        with jax.named_scope("fine"):
            squares = jnp.zeros((8, 128), F32)
            for g in range(GROUPS):
                own = r.grad[g, :64, :128]
                squares = squares + jnp.sum((own * own).reshape(8, 8, 128), axis=0)
                part = dot(r.sxf[:, :112], r.grad[g].astype(BF))
                for k in range(5):
                    r.u_fwd[k, g * 80 : g * 80 + 80] = part[k * 80 : k * 80 + 80].astype(BF)
            total = summed(r.u_fwd, r.syf, 0, GROUPS * 80)
            r.coarse[...] = (total * S_SCALE).astype(BF)
            r.fine[...] = dot(r.coarse[...], r.pyf[...]).astype(BF)

        @pl.loop(0, CHUNKS)
        @jax.named_scope("inc")
        def _(c):
            rows = pl.ds(pl.multiple_of(c * CHUNK, CHUNK), CHUNK)
            for g in range(GROUPS):
                part = dot(r.pxf[c, :, :80], r.fine[g * 80 : g * 80 + 80]).astype(BF)
                for l in range(LEV):
                    r.wbuf[c, l, g] = part[:, l * 128 : l * 128 + 128]
            for step, away in enumerate((2, 1, 3, 0)):
                level = lax.rem(mem + away, n_mem)
                sums = [jnp.zeros((CHUNK, 128), F32) for _ in range(VARS)]
                for m in range(GROUPS * PER):
                    place = slice(m % PER * CHUNK, m % PER * CHUNK + CHUNK)
                    weight = r.wbuf[c, level, m // PER, place].astype(F32)
                    for v in range(VARS):
                        sums[v] = sums[v] + r.ens[m, v, level, rows].astype(F32) * weight
                for v in range(VARS):
                    if away:
                        r.rs_send[it, c, step, v] = sums[v].astype(BF)
                    else:
                        r.rs_own[c, v] = sums[v]
                if away:
                    send(
                        r.rs_send.at[it, c, step], r.rs_recv.at[it, c, step],
                        r.rss_sem.at[it], r.rsr_sem.at[it, c], at(d_mem=away),
                    )

        def misfit_rows(c, energy):
            with jax.named_scope("w_rs"):
                wait(r.rs_recv.at[it, c], r.rsr_sem.at[it, c])
            rows = pl.ds(pl.multiple_of(c * CHUNK, CHUNK), CHUNK)
            for v in range(VARS):
                total = r.rs_own[c, v]
                for step in range(3):
                    total = total + r.rs_recv[it, c, step, v].astype(F32)
                total = total * scale
                rounded = (r.hub[v, mem, rows] * total).astype(BF)
                r.mis[it + 1, c, mem, v] = rounded
                product = rounded.astype(F32) * total
                energy = energy + product[:8] + product[8:]
            for away in (2, 1, 3):
                send(
                    r.mis.at[it + 1, c, mem], r.mis.at[it + 1, c, mem],
                    r.ags_sem.at[it], r.agr_sem.at[it, c], at(d_mem=away),
                )
            return energy

        energy = lax.fori_loop(0, CHUNKS, misfit_rows, jnp.zeros((8, 128), F32))
        squares = jnp.sum(squares, axis=0, keepdims=True)
        energy = jnp.sum(energy, axis=0, keepdims=True)
        r.sc_send[it, 0] = jnp.where(row8 == 0, squares, jnp.where(row8 == 1, energy, 0.0))
        scalar_send(it, 0, r.sc_a, plane)

        @pl.loop(0, CHUNKS - 1)
        def _(c):
            with jax.named_scope("w_ag"):
                wait(r.rs_recv.at[it, c], r.agr_sem.at[it, c])

            with jax.named_scope("adj"):
                @pl.loop(0, GROUPS)
                def _(g):
                    spread_rows(it + 1, c, g)

        with jax.named_scope("w_ag"):
            wait(r.rs_recv.at[it, CHUNKS - 1], r.agr_sem.at[it, CHUNKS - 1])

        with jax.named_scope("adj_send"):
            for groups in BATCHES:
                for g in groups:
                    spread_rows(it + 1, CHUNKS - 1, g)
                for g in groups:
                    coarse_rows(it + 1, g)
                coarse_send(it + 1, groups)

        r.sc_send[it, 1] = scalar_sum(it, 0, r.sc_a, len(plane))
        scalar_send(it, 1, r.sc_b, line)

        def store_image(g, value):
            r.ag[g] = value

        with jax.named_scope("post"):
            smoothed(it + 1, store_image)

        sums = scalar_sum(it, 1, r.sc_b, len(line))
        sums = jnp.sum(sums, axis=1, keepdims=True)
        squares, energy = sums[0:1], sums[1:2]
        alpha = squares / (squares + energy)

        with jax.named_scope("upd"):
            for g in range(GROUPS):
                gradient = r.grad[g]
                r.ctl[g] = r.ctl[g] - alpha * gradient[:64, :128]
                r.grad[g] = gradient - alpha * (gradient + r.ag[g])

    for g in range(GROUPS):
        r.out_c[g] = r.ctl[g]
        r.out_g[g] = r.grad[g, :64, :128]

    wait(r.h_recv.at[0], r.hs_sem.at[0])
    wait(r.l_recv.at[0], r.ls_sem.at[0])
    wait(r.d_recv.at[0], r.ds_sem.at[0])
    for it in range(ITERS):
        wait(r.h_recv.at[it + 1, pl.ds(0, GROUPS)], r.hs_sem.at[it + 1])
        wait(r.l_recv.at[it + 1, pl.ds(0, GROUPS)], r.ls_sem.at[it + 1])
        wait(r.d_recv.at[it + 1, pl.ds(0, GROUPS)], r.ds_sem.at[it + 1])
        wait(r.rs_recv.at[it], r.rss_sem.at[it])
        wait(r.rs_recv.at[it], r.ags_sem.at[it])
        wait(r.sc_a.at[it], r.scs_sem.at[it, 0])
        wait(r.sc_b.at[it], r.scs_sem.at[it, 1])


def unpack(control, gradient, out_c, out_g, spread, out_sem):
    backs = []
    for i, (packed, out) in enumerate(((control, out_c), (gradient, out_g))):
        for g in range(GROUPS):
            for l in range(LEV):
                turned = pltpu.roll(packed[g], 128 - 32 * l, 1) if l else packed[g]
                for m in range(PER):
                    spread[i, g * PER + m, l] = turned[m * 16 : m * 16 + 16, :32]
            members = pl.ds(g * PER, PER)
            backs.append(pltpu.make_async_copy(spread.at[i, members], out.at[members], out_sem.at[i, g]))
            backs[-1].start()
    for back in backs:
        back.wait()


def local(sizes, ensemble, huber, innovation, sea_mask):
    n_lon, n_lat, n_mem = sizes
    vmem, dma = pltpu.VMEM, pltpu.SemaphoreType.DMA
    shapes = {n: TABLES[n].shape[1:] if n in BY_LON + BY_LAT else TABLES[n].shape for n in NAMES}
    field = (VARS, FINE_X, FINE_Y)
    rows = (VARS, CHUNK, FINE_Y)
    times = ITERS + 1
    scratch = [
        vmem((MEMBERS // n_mem, VARS, LEV, FINE_X, FINE_Y), BF),
        vmem((LEV, *field), F32),
        vmem((LEV, *field), F32),
        vmem((OWN_X, OWN_Y), jnp.int32),
        *(vmem(shapes[n], BF) for n in NAMES),
        vmem((5, 256, 256), BF),
        vmem((5, 256, 256), BF),
        vmem((112, 256), F32),
        vmem((GROUPS, 112, 256), F32),
        vmem((GROUPS, 112, 256), F32),
        vmem((GROUPS, 64, 128), F32),
        vmem((5, GROUPS * 80, 256), BF),
        vmem((5, GROUPS * 112, 256), BF),
        vmem((GROUPS * 80, 256), BF),
        vmem((GROUPS * 80, 512), BF),
        vmem((CHUNKS, LEV, GROUPS, 64, 128), BF),
        vmem((GROUPS, 256, 512), BF),
        vmem((GROUPS * 80, 512), BF),
        vmem((times, CHUNKS, LEV, *rows), BF),
        vmem((CHUNKS, *rows), F32),
        vmem((ITERS, CHUNKS, 3, *rows), BF),
        vmem((ITERS, CHUNKS, 3, *rows), BF),
        vmem((times, GROUPS + 1, 4, 40, 128), BF),
        vmem((times, GROUPS + 1, 4, 40, 128), BF),
        vmem((times, GROUPS + 1, 2, 32, 128), BF),
        vmem((times, GROUPS + 1, 2, 32, 128), BF),
        vmem((times, GROUPS + 1, 4, 16, 128), BF),
        vmem((times, GROUPS + 1, 4, 16, 128), BF),
        vmem((ITERS, 2, 8, 128), F32),
        vmem((ITERS, n_mem * n_lat - 1, 8, 128), F32),
        vmem((ITERS, n_lon - 1, 8, 128), F32),
        dma((len(NAMES) + 3,)),
        dma((GROUPS,)),
        dma((times,)),
        dma((times, GROUPS + 1)),
        dma((times,)),
        dma((times, GROUPS + 1)),
        dma((times,)),
        dma((times, GROUPS + 1)),
        dma((ITERS,)),
        dma((ITERS, CHUNKS)),
        dma((ITERS,)),
        dma((ITERS, CHUNKS)),
        dma((ITERS, 2)),
        dma((ITERS, 2)),
    ]
    packed = jax.ShapeDtypeStruct((GROUPS, PER * OWN_X, 128), F32)
    any_space, in_vmem = pl.BlockSpec(memory_space=pl.ANY), pl.BlockSpec(memory_space=pltpu.VMEM)
    control, gradient = pl.pallas_call(
        lambda *refs: kernel(sizes, *refs),
        out_shape=(vmem(packed.shape, F32),) * 2,
        in_specs=[pl.BlockSpec(memory_space=pltpu.HBM)] * (4 + len(NAMES)),
        out_specs=(in_vmem, in_vmem),
        scratch_shapes=scratch,
        name="assimilate",
        compiler_params=pltpu.CompilerParams(collective_id=0, has_side_effects=True, vmem_limit_bytes=60 * 2**20),
    )(ensemble, huber, innovation, sea_mask, *(jnp.asarray(TABLES[n]) for n in NAMES))
    out = jax.ShapeDtypeStruct((MEMBERS // n_mem, LEV, OWN_X, OWN_Y), F32)
    return pl.pallas_call(
        unpack,
        out_shape=(out, out),
        in_specs=[in_vmem] * 2,
        out_specs=(any_space, any_space),
        scratch_shapes=[
            vmem((2, *out.shape), F32),
            dma((2, GROUPS)),
        ],
        name="unpack",
        compiler_params=pltpu.CompilerParams(vmem_limit_bytes=8 * 2**20),
    )(control, gradient)


def solution(mesh):
    sizes = tuple(mesh.shape[name] for name in ("lon", "lat", "mem"))
    in_specs = (
        P("mem", None, None, "lon", "lat"),
        P(None, None, "lon", "lat"),
        P(None, None, "lon", "lat"),
        P("lon", "lat"),
    )
    out_specs = (P("mem", None, "lon", "lat"), P("mem", None, "lon", "lat"))
    return jax.shard_map(
        lambda *args: local(sizes, *args), mesh=mesh, in_specs=in_specs, out_specs=out_specs, check_vma=False
    )
```
